256 devices in a mesh: row: 16 (over x_hi, z), col: 16 (over x_lo, y, core).
Axes of the slice: x: 4 (x_hi: 2, x_lo: 2; x = x_hi * 2 + x_lo), y: 4, z: 8, core: 2. Of those that a mesh axis runs over, the one named last changes fastest.
Arguments:
- pair: bfloat16 [512, 512, 128], P('row', 'col'), may hold values from -6 to 6
- norm_in: float32 [128], replicated, may hold values from 0.1 to 1.9
- shift_in: float32 [128], replicated, may hold values from -3 to 3
- in_weight: bfloat16 [128, 640], replicated, may hold values from -0.5 to 0.5
- norm_out: float32 [128], replicated, may hold values from 0.1 to 1.9
- shift_out: float32 [128], replicated, may hold values from -3 to 3
- out_weight: bfloat16 [128, 128], replicated, may hold values from -0.5 to 0.5
Outputs:
- update: bfloat16 [512, 512, 128], P('row', 'col')
The draws below stay inside these ranges and needn't reach their ends.
All inputs are finite; a program needn't handle non-finite values.
Results may differ from the reference program's by a relative error of at most 0.0054.
Values may be sent and summed in bfloat16 or wider, within the bound.
No kernel may reach another device: no remote copies, remote signals or barrier semaphores. Data moves between devices by JAX's collectives and lax.ppermute only.
A program may use at most 64 MiB of HBM per device.

```python
import jax
import jax.numpy as jnp
from jax import lax

C = 128
CH = 128
N = 512
ROWS = 32
N_ROW = 16


def block_levels(key, extent, split, smallest, high):
    loudness, own = 1.0, jax.random.fold_in(key, 6)
    for dim, blocks in split:
        heights = jnp.exp(jax.random.uniform(jax.random.fold_in(own, dim), (blocks,), jnp.float32, smallest / len(split), high / len(split)))
        loudness = loudness * jnp.repeat(heights, extent[dim] // blocks).reshape([-1 if axis == dim else 1 for axis in range(len(extent))])
    return loudness


def centred(key, extent, scale, bound, pieces=(), held_as=jnp.bfloat16):
    result = jax.random.normal(key, extent, jnp.float32) * scale
    if len(pieces) > 0:
        result = block_levels(key, extent, pieces, -0.22, 0.18) * result
    return jnp.clip(result, min=-bound, max=bound).astype(held_as)


def setup_inputs(seed: int = 0) -> dict:
    streams_of = jax.random.split(jax.random.key(seed), 8)
    return {
        "pair": centred(streams_of[0], (N, N, C), 1.0, 6.0, ((0, 16), (1, 16))),
        "norm_in": jnp.clip(1.0 + 0.18 * jax.random.normal(streams_of[1], (C,), jnp.float32), 0.1, 1.9),
        "shift_in": centred(streams_of[2], (C,), 0.5, 3.0, (), jnp.float32),
        "in_weight": centred(streams_of[3], (C, 4 * CH + C), C ** -0.5, 0.5),
        "norm_out": jnp.clip(1.0 + 0.18 * jax.random.normal(streams_of[4], (CH,), jnp.float32), 0.1, 1.9),
        "shift_out": centred(streams_of[5], (CH,), 0.5, 3.0, (), jnp.float32),
        "out_weight": centred(streams_of[6], (CH, C), CH ** -0.5, 0.5),
    }


EPSILON = 1e-05

def layer_norm(values, gain, shift):
    values = values.astype(jnp.float32)
    center = lax.optimization_barrier(jnp.mean(values, axis=-1, keepdims=True))
    spread = lax.optimization_barrier(jnp.mean(jnp.square(values - center), axis=-1, keepdims=True))
    return (values - center) * lax.rsqrt(spread + EPSILON) * gain + shift

def project_block(block, norm_in, shift_in, in_weight):
    normed = layer_norm(block, norm_in, shift_in).astype(jnp.bfloat16)
    projected = jnp.dot(normed.reshape(-1, C), in_weight, preferred_element_type=jnp.float32)
    left = (jax.nn.sigmoid(projected[:, :CH]) * projected[:, CH:2 * CH]).astype(jnp.bfloat16)
    right = (jax.nn.sigmoid(projected[:, 2 * CH:3 * CH]) * projected[:, 3 * CH:4 * CH]).astype(jnp.bfloat16)
    gate = jax.nn.sigmoid(projected[:, 4 * CH:])
    return (left, right, gate)

def reference(pair, norm_in, shift_in, in_weight, norm_out, shift_out, out_weight):
    blocks = pair.reshape(N_ROW, ROWS, N, C)
    left, right, gate = lax.map(lambda block: project_block(block, norm_in, shift_in, in_weight), blocks)
    left = left.reshape(N, N, CH).astype(jnp.float32)
    right = right.reshape(N, N, CH).astype(jnp.float32)
    gate = gate.reshape(N, N, C)
    mixed = jnp.einsum('kih,kjh->ijh', left, right)
    mixed_normed = layer_norm(mixed, norm_out, shift_out).astype(jnp.bfloat16)
    outward = jnp.dot(mixed_normed.reshape(-1, CH), out_weight, preferred_element_type=jnp.float32)
    return (gate * outward.reshape(N, N, C)).astype(jnp.bfloat16)
```

```python
import jax
import jax.numpy as jnp
from jax import lax
from jax.experimental import pallas as pl
from jax.experimental.pallas import tpu as pltpu
from jax.sharding import Mesh, PartitionSpec as P

EPSILON = 1e-05
CHIPS = ("xh", "z", "xl", "y")
F32 = jnp.float32
BF16 = jnp.bfloat16
VMEM = pl.BlockSpec(memory_space=pltpu.VMEM)
SMEM = pl.BlockSpec(memory_space=pltpu.SMEM)


def swap_groups(v):
    lane = lax.broadcasted_iota(jnp.int32, v[0].shape, 1)
    low = lane < 64
    u = [None] * 4
    for c in (0, 1):
        a, b = v[c], v[c + 2]
        u[c] = jnp.where(low, a, pltpu.roll(b, 64, 1))
        u[c + 2] = jnp.where(low, pltpu.roll(a, 64, 1), b)
    even = (lane & 32) == 0
    out = [None] * 4
    for c in (0, 2):
        a, b = u[c], u[c + 1]
        out[c] = jnp.where(even, a, pltpu.roll(b, 32, 1))
        out[c + 1] = jnp.where(even, pltpu.roll(a, 96, 1), b)
    return out


def project_kernel(pair_ref, gain_ref, shift_ref, w_ref, msg_ref, normed_ref, scr_ref):
    gain = gain_ref[...]
    shift = shift_ref[...]
    wt = jnp.transpose(w_ref[:, :512].astype(F32)).astype(BF16)
    for a in range(8):
        x = pair_ref[a * 128 : (a + 1) * 128, :].astype(F32)
        center = jnp.mean(x, axis=-1, keepdims=True)
        d = x - center
        spread = jnp.mean(d * d, axis=-1, keepdims=True)
        n = (d * lax.rsqrt(spread + EPSILON) * gain + shift).astype(BF16)
        normed_ref[a * 128 : (a + 1) * 128, :] = n
        p = lax.dot_general(wt, n, (((1,), (1,)), ((), ())), preferred_element_type=F32)
        left = jax.nn.sigmoid(p[0:128]) * p[128:256]
        right = jax.nn.sigmoid(p[256:384]) * p[384:512]
        scr_ref[pl.ds(a, 128, stride=16), :] = left
        scr_ref[pl.ds(8 + a, 128, stride=16), :] = right
    msg_ref[...] = scr_ref[...].astype(BF16)


def gate_kernel(normed_ref, w_ref, gate_ref):
    gate_ref[...] = jax.nn.sigmoid(
        jnp.dot(normed_ref[...], w_ref[:, 512:640], preferred_element_type=F32)
    )


def spread_kernel(offset, recv_ref, out_ref):
    for r in range(16):
        for g in range(2):
            base = (r * 8 + g * 4) * 16
            v = [
                recv_ref[base + c * 16 : base + c * 16 + 16, :].astype(F32)[offset : offset + 8]
                for c in range(4)
            ]
            out_ref[r * 32 : (r + 1) * 32, g * 128 : (g + 1) * 128] = jnp.concatenate(
                swap_groups(v), axis=0
            ).astype(BF16)


def mix_kernel(core_ref, own_ref, other_ref, right_ref, out_ref):
    core = core_ref[0]
    right = right_ref[...]
    for part, ref in ((core, own_ref), (1 - core, other_ref)):
        mixed = lax.dot_general(
            ref[...], right, (((0,), (0,)), ((), ())), preferred_element_type=F32
        )
        for q in range(8):
            row = 2 * q + part
            for g in range(2):
                v = mixed[q * 32 : (q + 1) * 32, g * 128 : (g + 1) * 128]
                v = [v[b * 8 : (b + 1) * 8] for b in range(4)]
                start = pl.multiple_of(row * 64 + g * 32, 32)
                out_ref[pl.ds(start, 32), :] = jnp.concatenate(swap_groups(v), axis=0).astype(BF16)


def output_kernel(recv_ref, gate_ref, gain_ref, shift_ref, w_ref, out_ref, scr_ref):
    total = jnp.zeros((8, 128), F32)
    for t in range(64):
        x = recv_ref[t * 16 : (t + 1) * 16, :].astype(F32)
        total = total + x[0:8] + x[8:16]
    center = total * (1.0 / 128.0)
    square = jnp.zeros((8, 128), F32)
    for t in range(64):
        x = recv_ref[t * 16 : (t + 1) * 16, :].astype(F32)
        d0 = x[0:8] - center
        d1 = x[8:16] - center
        square = square + d0 * d0 + d1 * d1
    scale = lax.rsqrt(square * (1.0 / 128.0) + EPSILON)
    for t in range(64):
        x = recv_ref[t * 16 : (t + 1) * 16, :].astype(F32)
        for k in range(2):
            h = 2 * t + k
            scr_ref[h * 8 : (h + 1) * 8, :] = (x[k * 8 : k * 8 + 8] - center) * scale * gain_ref[
                h
            ] + shift_ref[h]
    w = w_ref[...]
    for s in range(8):
        x = scr_ref[pl.ds(s, 128, stride=8), :].astype(BF16)
        o = lax.dot_general(x, w, (((0,), (0,)), ((), ())), preferred_element_type=F32)
        for b in range(4):
            i = b * 8 + s
            rows = slice(i * 32, (i + 1) * 32)
            out_ref[rows, :] = (gate_ref[rows, :] * o[b * 32 : (b + 1) * 32]).astype(BF16)


def local(pair, norm_in, shift_in, in_weight, norm_out, shift_out, out_weight):
    core = lax.axis_index("core").astype(jnp.int32).reshape(1)
    msg, normed = pl.pallas_call(
        project_kernel,
        out_shape=(
            jax.ShapeDtypeStruct((2048, 128), BF16),
            jax.ShapeDtypeStruct((1024, 128), BF16),
        ),
        in_specs=[VMEM] * 4,
        out_specs=(VMEM, VMEM),
        scratch_shapes=[pltpu.VMEM((2048, 128), F32)],
        name="project",
    )(pair.reshape(1024, 128), norm_in.reshape(1, 128), shift_in.reshape(1, 128), in_weight)
    recv = lax.all_to_all(msg.reshape(128, 16, 128), CHIPS, 0, 0, tiled=True).reshape(2048, 128)
    gate = pl.pallas_call(
        gate_kernel,
        out_shape=jax.ShapeDtypeStruct((1024, 128), F32),
        in_specs=[VMEM] * 2,
        out_specs=VMEM,
        name="gate",
        cost_estimate=pl.CostEstimate(flops=1 << 25, bytes_accessed=1 << 20, transcendentals=1 << 17),
    )(normed, in_weight)

    def spread(offset, name):
        return pl.pallas_call(
            lambda a, b: spread_kernel(offset, a, b),
            out_shape=jax.ShapeDtypeStruct((512, 256), BF16),
            in_specs=[VMEM],
            out_specs=VMEM,
            name=name,
            cost_estimate=pl.CostEstimate(flops=1 << 22, bytes_accessed=1 << 20, transcendentals=0),
        )(recv)

    own = spread(0, "spread_left")
    other = lax.ppermute(own, "core", [(0, 1), (1, 0)])
    right = spread(8, "spread_right")
    back = pl.pallas_call(
        mix_kernel,
        out_shape=jax.ShapeDtypeStruct((1024, 128), BF16),
        in_specs=[SMEM, VMEM, VMEM, VMEM],
        out_specs=VMEM,
        name="mix",
    )(core, own, other, right)
    mixed = lax.all_to_all(back.reshape(128, 8, 128), CHIPS, 0, 0, tiled=True).reshape(1024, 128)
    out = pl.pallas_call(
        output_kernel,
        out_shape=jax.ShapeDtypeStruct((1024, 128), BF16),
        in_specs=[VMEM, VMEM, SMEM, SMEM, VMEM],
        out_specs=VMEM,
        scratch_shapes=[pltpu.VMEM((1024, 128), F32)],
        name="output",
    )(mixed, gate, norm_out, shift_out, out_weight)
    return out.reshape(pair.shape)


def solution(mesh):
    fine = Mesh(mesh.devices.reshape(2, 8, 2, 4, 2), ("xh", "z", "xl", "y", "core"))
    spec = P(("xh", "z"), ("xl", "y", "core"), None)
    in_specs = (spec, P(), P(), P(), P(), P(), P())
    return jax.shard_map(local, mesh=fine, in_specs=in_specs, out_specs=spec, check_vma=False)
```

```python
import jax
import jax.numpy as jnp
from jax import lax
from jax.experimental import pallas as pl
from jax.experimental.pallas import tpu as pltpu
from jax.sharding import Mesh, PartitionSpec as P

EPSILON = 1e-05
CHIPS = ("xh", "z", "xl", "y")
F32 = jnp.float32
BF16 = jnp.bfloat16
VMEM = pl.BlockSpec(memory_space=pltpu.VMEM)
SMEM = pl.BlockSpec(memory_space=pltpu.SMEM)
SMALL = pltpu.CompilerParams(vmem_limit_bytes=12 << 20)


def swap_groups(v):
    lane = lax.broadcasted_iota(jnp.int32, v[0].shape, 1)
    low = lane < 64
    u = [None] * 4
    for c in (0, 1):
        a, b = v[c], v[c + 2]
        u[c] = jnp.where(low, a, pltpu.roll(b, 64, 1))
        u[c + 2] = jnp.where(low, pltpu.roll(a, 64, 1), b)
    even = (lane & 32) == 0
    out = [None] * 4
    for c in (0, 2):
        a, b = u[c], u[c + 1]
        out[c] = jnp.where(even, a, pltpu.roll(b, 32, 1))
        out[c + 1] = jnp.where(even, pltpu.roll(a, 96, 1), b)
    return out


def project_kernel(pair_ref, gain_ref, shift_ref, w_ref, msg_ref, normed_ref, scr_ref):
    gain = gain_ref[...]
    shift = shift_ref[...]
    wt = jnp.transpose(w_ref[:, :512].astype(F32)).astype(BF16)
    for a in range(8):
        x = pair_ref[a * 128 : (a + 1) * 128, :].astype(F32)
        center = jnp.mean(x, axis=-1, keepdims=True)
        d = x - center
        spread = jnp.mean(d * d, axis=-1, keepdims=True)
        n = (d * lax.rsqrt(spread + EPSILON) * gain + shift).astype(BF16)
        normed_ref[a * 128 : (a + 1) * 128, :] = n
        p = lax.dot_general(wt, n, (((1,), (1,)), ((), ())), preferred_element_type=F32)
        left = jax.nn.sigmoid(p[0:128]) * p[128:256]
        right = jax.nn.sigmoid(p[256:384]) * p[384:512]
        scr_ref[pl.ds(a, 128, stride=16), :] = left
        scr_ref[pl.ds(8 + a, 128, stride=16), :] = right
    msg_ref[...] = scr_ref[...].astype(BF16)


def gate_kernel(normed_ref, w_ref, gate_ref):
    gate_ref[...] = jax.nn.sigmoid(
        jnp.dot(normed_ref[...], w_ref[:, 512:640], preferred_element_type=F32)
    )


def spread(recv_ref, offset):
    out = []
    for r in range(16):
        halves = []
        for g in range(2):
            base = (r * 8 + g * 4) * 16
            v = [
                recv_ref[base + c * 16 : base + c * 16 + 16, :].astype(F32)[offset : offset + 8]
                for c in range(4)
            ]
            halves.append(jnp.concatenate(swap_groups(v), axis=0).astype(BF16))
        out.append(halves)
    return out


def gather_pieces(mixed, q, g):
    v = mixed[q * 32 : (q + 1) * 32, g * 128 : (g + 1) * 128]
    v = [v[b * 8 : (b + 1) * 8] for b in range(4)]
    return jnp.concatenate(swap_groups(v), axis=0).astype(BF16)


def store_spread(recv_ref, offset, out_ref):
    for r, halves in enumerate(spread(recv_ref, offset)):
        for g in range(2):
            out_ref[r * 32 : (r + 1) * 32, g * 128 : (g + 1) * 128] = halves[g]


def own_kernel(recv_ref, right_ref, out_ref, left_ref):
    store_spread(recv_ref, 0, left_ref)
    store_spread(recv_ref, 8, right_ref)
    mixed = lax.dot_general(
        left_ref[...], right_ref[...], (((0,), (0,)), ((), ())), preferred_element_type=F32
    )
    for q in range(8):
        for g in range(2):
            out_ref[q * 64 + g * 32 : q * 64 + g * 32 + 32, :] = gather_pieces(mixed, q, g)


def other_kernel(core_ref, recv_ref, right_ref, own_ref, out_ref, left_ref):
    core = core_ref[0]
    for q in range(8):
        start = pl.multiple_of((2 * q + core) * 64, 64)
        out_ref[pl.ds(start, 64), :] = own_ref[q * 64 : (q + 1) * 64, :]
    store_spread(recv_ref, 0, left_ref)
    mixed = lax.dot_general(
        left_ref[...], right_ref[...], (((0,), (0,)), ((), ())), preferred_element_type=F32
    )
    for q in range(8):
        for g in range(2):
            start = pl.multiple_of((2 * q + 1 - core) * 64 + g * 32, 32)
            out_ref[pl.ds(start, 32), :] = gather_pieces(mixed, q, g)


def output_kernel(recv_ref, gate_ref, gain_ref, shift_ref, w_ref, out_ref, scr_ref):
    total = jnp.zeros((8, 128), F32)
    for t in range(64):
        x = recv_ref[t * 16 : (t + 1) * 16, :].astype(F32)
        total = total + x[0:8] + x[8:16]
    center = total * (1.0 / 128.0)
    square = jnp.zeros((8, 128), F32)
    for t in range(64):
        x = recv_ref[t * 16 : (t + 1) * 16, :].astype(F32)
        d0 = x[0:8] - center
        d1 = x[8:16] - center
        square = square + d0 * d0 + d1 * d1
    scale = lax.rsqrt(square * (1.0 / 128.0) + EPSILON)
    for t in range(64):
        x = recv_ref[t * 16 : (t + 1) * 16, :].astype(F32)
        for k in range(2):
            h = 2 * t + k
            scr_ref[h * 8 : (h + 1) * 8, :] = (x[k * 8 : k * 8 + 8] - center) * scale * gain_ref[
                h
            ] + shift_ref[h]
    w = w_ref[...]
    for s in range(8):
        x = scr_ref[pl.ds(s, 128, stride=8), :].astype(BF16)
        o = lax.dot_general(x, w, (((0,), (0,)), ((), ())), preferred_element_type=F32)
        for b in range(4):
            i = b * 8 + s
            rows = slice(i * 32, (i + 1) * 32)
            out_ref[rows, :] = (gate_ref[rows, :] * o[b * 32 : (b + 1) * 32]).astype(BF16)


def local(pair, norm_in, shift_in, in_weight, norm_out, shift_out, out_weight):
    core = lax.axis_index("core").astype(jnp.int32).reshape(1)
    msg, normed = pl.pallas_call(
        project_kernel,
        out_shape=(
            jax.ShapeDtypeStruct((2048, 128), BF16),
            jax.ShapeDtypeStruct((1024, 128), BF16),
        ),
        in_specs=[VMEM] * 4,
        out_specs=(VMEM, VMEM),
        scratch_shapes=[pltpu.VMEM((2048, 128), F32)],
        compiler_params=SMALL,
        name="project",
    )(pair.reshape(1024, 128), norm_in.reshape(1, 128), shift_in.reshape(1, 128), in_weight)
    recv = lax.all_to_all(msg.reshape(128, 16, 128), CHIPS, 0, 0, tiled=True).reshape(2048, 128)
    gate = pl.pallas_call(
        gate_kernel,
        out_shape=jax.ShapeDtypeStruct((1024, 128), F32),
        in_specs=[VMEM] * 2,
        out_specs=VMEM,
        compiler_params=SMALL,
        name="gate",
        cost_estimate=pl.CostEstimate(flops=1 << 25, bytes_accessed=1 << 20, transcendentals=1 << 17),
    )(normed, in_weight)

    other = lax.ppermute(recv, "core", [(0, 1), (1, 0)])
    right, own = pl.pallas_call(
        own_kernel,
        out_shape=(
            jax.ShapeDtypeStruct((512, 256), BF16),
            jax.ShapeDtypeStruct((512, 128), BF16),
        ),
        in_specs=[VMEM],
        out_specs=(VMEM, VMEM),
        scratch_shapes=[pltpu.VMEM((512, 256), BF16)],
        compiler_params=SMALL,
        name="own",
        cost_estimate=pl.CostEstimate(flops=1 << 26, bytes_accessed=1 << 20, transcendentals=0),
    )(recv)
    back = pl.pallas_call(
        other_kernel,
        out_shape=jax.ShapeDtypeStruct((1024, 128), BF16),
        in_specs=[SMEM, VMEM, VMEM, VMEM],
        out_specs=VMEM,
        scratch_shapes=[pltpu.VMEM((512, 256), BF16)],
        compiler_params=SMALL,
        name="other",
    )(core, other, right, own)
    mixed = lax.all_to_all(back.reshape(128, 8, 128), CHIPS, 0, 0, tiled=True).reshape(1024, 128)
    out = pl.pallas_call(
        output_kernel,
        out_shape=jax.ShapeDtypeStruct((1024, 128), BF16),
        in_specs=[VMEM, VMEM, SMEM, SMEM, VMEM],
        out_specs=VMEM,
        scratch_shapes=[pltpu.VMEM((1024, 128), F32)],
        compiler_params=SMALL,
        name="output",
    )(mixed, gate, norm_out, shift_out, out_weight)
    return out.reshape(pair.shape)


def solution(mesh):
    fine = Mesh(mesh.devices.reshape(2, 8, 2, 4, 2), ("xh", "z", "xl", "y", "core"))
    spec = P(("xh", "z"), ("xl", "y", "core"), None)
    in_specs = (spec, P(), P(), P(), P(), P(), P())
    return jax.shard_map(local, mesh=fine, in_specs=in_specs, out_specs=spec, check_vma=False)
```

```python
import functools

import jax
import jax.numpy as jnp
from jax import lax
from jax.experimental import pallas as pl
from jax.experimental.pallas import tpu as pltpu
from jax.sharding import Mesh, PartitionSpec as P

EPSILON = 1e-05
CHIPS = ("xh", "z", "xl", "y")
F32 = jnp.float32
BF16 = jnp.bfloat16
VMEM = pl.BlockSpec(memory_space=pltpu.VMEM)
SMEM = pl.BlockSpec(memory_space=pltpu.SMEM)
HBM = pl.BlockSpec(memory_space=pltpu.HBM)
UNROLL = 8
SMALL = pltpu.CompilerParams(vmem_limit_bytes=12 << 20)


def swap_groups(v):
    lane = lax.broadcasted_iota(jnp.int32, v[0].shape, 1)
    low = lane < 64
    u = [None] * 4
    for c in (0, 1):
        a, b = v[c], v[c + 2]
        u[c] = jnp.where(low, a, pltpu.roll(b, 64, 1))
        u[c + 2] = jnp.where(low, pltpu.roll(a, 64, 1), b)
    even = (lane & 32) == 0
    out = [None] * 4
    for c in (0, 2):
        a, b = u[c], u[c + 1]
        out[c] = jnp.where(even, a, pltpu.roll(b, 32, 1))
        out[c + 1] = jnp.where(even, pltpu.roll(a, 96, 1), b)
    return out


def project_kernel(
    pair_hbm,
    gain_hbm,
    shift_hbm,
    w_hbm,
    gain_out_hbm,
    shift_out_hbm,
    w_out_hbm,
    msg_ref,
    gate_ref,
    gain_col_ref,
    shift_col_ref,
    w_out_ref,
    pair_ref,
    w_ref,
    rows_ref,
    scr_ref,
    sem,
):
    def pair_copy(t):
        rows = slice(t * 256, (t + 1) * 256)
        return pltpu.make_async_copy(pair_hbm.at[rows], pair_ref.at[rows], sem.at[6 + t])

    w_copy = pltpu.make_async_copy(w_hbm, w_ref, sem.at[0])
    small = [
        pltpu.make_async_copy(ref, rows_ref.at[pl.ds(t * 8, 1)], sem.at[1 + t])
        for t, ref in enumerate((gain_hbm, shift_hbm, gain_out_hbm, shift_out_hbm))
    ]
    w_out_copy = pltpu.make_async_copy(w_out_hbm, w_out_ref, sem.at[5])
    w_copy.start()
    small[0].start()
    small[1].start()
    for t in range(4):
        pair_copy(t).start()
    small[2].start()
    small[3].start()
    w_out_copy.start()
    w_copy.wait()
    wt = jnp.transpose(w_ref[:, :512].astype(F32)).astype(BF16)
    wg = w_ref[:, 512:640]
    small[0].wait()
    small[1].wait()
    gain = rows_ref[0:1, :]
    shift = rows_ref[8:9, :]
    for a in range(8):
        if a % 2 == 0:
            pair_copy(a // 2).wait()
        x = pair_ref[a * 128 : (a + 1) * 128, :].astype(F32)
        center = jnp.mean(x, axis=-1, keepdims=True)
        d = x - center
        spread = jnp.mean(d * d, axis=-1, keepdims=True)
        n = (d * lax.rsqrt(spread + EPSILON) * gain + shift).astype(BF16)
        p = lax.dot_general(wt, n, (((1,), (1,)), ((), ())), preferred_element_type=F32)
        left = jax.nn.sigmoid(p[0:128]) * p[128:256]
        right = jax.nn.sigmoid(p[256:384]) * p[384:512]
        scr_ref[pl.ds(a, 128, stride=16), :] = left
        scr_ref[pl.ds(8 + a, 128, stride=16), :] = right
        gate_ref[a * 128 : (a + 1) * 128, :] = jax.nn.sigmoid(
            jnp.dot(n, wg, preferred_element_type=F32)
        )
    msg_ref[...] = scr_ref[...].astype(BF16)
    small[2].wait()
    small[3].wait()
    gain_col_ref[...] = jnp.transpose(jnp.broadcast_to(rows_ref[16:17, :], (128, 128)))
    shift_col_ref[...] = jnp.transpose(jnp.broadcast_to(rows_ref[24:25, :], (128, 128)))
    w_out_copy.wait()


def spread_kernel(offset, recv_ref, out_ref):
    def step(t, carry):
        for u in range(UNROLL):
            r = t * UNROLL + u
            for g in range(2):
                base = r * 128 + g * 64
                v = []
                for c in range(4):
                    start = pl.multiple_of(base + c * 16, 16)
                    piece = recv_ref[pl.ds(start, 16), :].astype(F32)
                    v.append(piece[offset : offset + 8])
                out_ref[pl.ds(pl.multiple_of(r * 32, 32), 32), g * 128 : (g + 1) * 128] = (
                    jnp.concatenate(swap_groups(v), axis=0).astype(BF16)
                )
        return carry

    lax.fori_loop(0, 16 // UNROLL, step, 0)


def multiply(left_ref, right_ref, mixed_ref):
    mixed_ref[...] = lax.dot_general(
        left_ref[...], right_ref[...], (((0,), (0,)), ((), ())), preferred_element_type=F32
    )


def pieces(mixed_ref, out_ref, row_of):
    def step(t, carry):
        for u in range(4):
            q = t * 4 + u
            for g in range(2):
                v = []
                for b in range(4):
                    start = pl.multiple_of(q * 32 + b * 8, 8)
                    v.append(mixed_ref[pl.ds(start, 8), g * 128 : (g + 1) * 128])
                start = pl.multiple_of(row_of(q) * 64 + g * 32, 32)
                out_ref[pl.ds(start, 32), :] = jnp.concatenate(swap_groups(v), axis=0).astype(BF16)
        return carry

    lax.fori_loop(0, 2, step, 0)


def own_kernel(recv_ref, left_ref, right_ref, out_ref, mixed_ref):
    spread_kernel(8, recv_ref, right_ref)
    multiply(left_ref, right_ref, mixed_ref)
    pieces(mixed_ref, out_ref, lambda q: q)


def other_kernel(core_ref, left_ref, right_ref, own_ref, out_ref, mixed_ref):
    core = core_ref[0]
    multiply(left_ref, right_ref, mixed_ref)
    for q in range(8):
        start = pl.multiple_of((2 * q + core) * 64, 64)
        out_ref[pl.ds(start, 64), :] = own_ref[q * 64 : (q + 1) * 64, :]
    pieces(mixed_ref, out_ref, lambda q: 2 * q + 1 - core)


def output_kernel(recv_ref, gate_ref, gain_ref, shift_ref, w_ref, out_ref, scr_ref):
    def total_step(t, sums):
        sums = list(sums)
        for u in range(16):
            rows = pl.ds(pl.multiple_of(t * 256 + u * 16, 16), 16)
            x = recv_ref[rows, :].astype(F32)
            scr_ref[rows, :] = x
            sums[u % 4] = sums[u % 4] + (x[0:8] + x[8:16])
        return tuple(sums)

    zero = jnp.zeros((8, 128), F32)
    sums = lax.fori_loop(0, 4, total_step, (zero,) * 4)
    center = ((sums[0] + sums[1]) + (sums[2] + sums[3])) * (1.0 / 128.0)

    def square_step(t, sums):
        sums = list(sums)
        for u in range(32):
            d = scr_ref[pl.ds(pl.multiple_of(t * 256 + u * 8, 8), 8), :] - center
            sums[u % 4] = sums[u % 4] + d * d
        return tuple(sums)

    sums = lax.fori_loop(0, 4, square_step, (zero,) * 4)
    spread = ((sums[0] + sums[1]) + (sums[2] + sums[3])) * (1.0 / 128.0)
    scale = lax.rsqrt(spread + EPSILON)
    w = w_ref[...]
    for s in range(8):
        x = scr_ref[pl.ds(s, 128, stride=8), :]
        x = (x - center[s : s + 1]) * scale[s : s + 1] * gain_ref[...] + shift_ref[...]
        o = lax.dot_general(
            x.astype(BF16), w, (((0,), (0,)), ((), ())), preferred_element_type=F32
        )
        for b in range(4):
            i = b * 8 + s
            rows = slice(i * 32, (i + 1) * 32)
            out_ref[rows, :] = (gate_ref[rows, :] * o[b * 32 : (b + 1) * 32]).astype(BF16)


def local(pair, norm_in, shift_in, in_weight, norm_out, shift_out, out_weight):
    core = lax.axis_index("core").astype(jnp.int32).reshape(1)
    shape = jax.ShapeDtypeStruct
    msg, gate, gain_col, shift_col, w_out = pl.pallas_call(
        project_kernel,
        out_shape=(
            shape((2048, 128), BF16),
            shape((1024, 128), F32),
            shape((128, 128), F32),
            shape((128, 128), F32),
            shape((128, 128), BF16),
        ),
        in_specs=[HBM] * 7,
        out_specs=(VMEM,) * 5,
        scratch_shapes=[
            pltpu.VMEM((1024, 128), BF16),
            pltpu.VMEM((128, 640), BF16),
            pltpu.VMEM((32, 128), F32),
            pltpu.VMEM((2048, 128), F32),
            pltpu.SemaphoreType.DMA((10,)),
        ],
        compiler_params=SMALL,
        name="project",
    )(
        pair.reshape(1024, 128),
        norm_in.reshape(1, 128),
        shift_in.reshape(1, 128),
        in_weight,
        norm_out.reshape(1, 128),
        shift_out.reshape(1, 128),
        out_weight,
    )
    recv = lax.all_to_all(msg.reshape(128, 16, 128), CHIPS, 0, 0, tiled=True).reshape(2048, 128)
    left = pl.pallas_call(
        functools.partial(spread_kernel, 0),
        out_shape=shape((512, 256), BF16),
        in_specs=[VMEM],
        out_specs=VMEM,
        compiler_params=SMALL,
        name="spread",
    )(recv)
    other = lax.ppermute(left, "core", [(0, 1), (1, 0)])
    right, own = pl.pallas_call(
        own_kernel,
        out_shape=(shape((512, 256), BF16), shape((512, 128), BF16)),
        in_specs=[VMEM, VMEM],
        out_specs=(VMEM, VMEM),
        scratch_shapes=[pltpu.VMEM((256, 256), F32)],
        compiler_params=SMALL,
        name="own",
        cost_estimate=pl.CostEstimate(flops=1 << 26, bytes_accessed=1 << 20, transcendentals=0),
    )(recv, left)
    back = pl.pallas_call(
        other_kernel,
        out_shape=shape((1024, 128), BF16),
        in_specs=[SMEM, VMEM, VMEM, VMEM],
        out_specs=VMEM,
        scratch_shapes=[pltpu.VMEM((256, 256), F32)],
        compiler_params=SMALL,
        name="other",
    )(core, other, right, own)
    mixed = lax.all_to_all(back.reshape(128, 8, 128), CHIPS, 0, 0, tiled=True).reshape(1024, 128)
    out = pl.pallas_call(
        output_kernel,
        out_shape=shape((1024, 128), BF16),
        in_specs=[VMEM] * 5,
        out_specs=VMEM,
        scratch_shapes=[pltpu.VMEM((1024, 128), F32)],
        compiler_params=SMALL,
        name="output",
    )(mixed, gate, gain_col, shift_col, w_out)
    return out.reshape(pair.shape)


def solution(mesh):
    fine = Mesh(mesh.devices.reshape(2, 8, 2, 4, 2), ("xh", "z", "xl", "y", "core"))
    spec = P(("xh", "z"), ("xl", "y", "core"), None)
    in_specs = (spec, P(), P(), P(), P(), P(), P())
    return jax.shard_map(local, mesh=fine, in_specs=in_specs, out_specs=spec, check_vma=False)
```

```python
import functools
import itertools

import jax
import jax.numpy as jnp
from jax import lax
from jax.experimental import pallas as pl
from jax.experimental.pallas import tpu as pltpu
from jax.sharding import Mesh, PartitionSpec as P

EPSILON = 1e-05
AXES = ("xh", "z", "xl", "y", "core")
ROOT = (1, 4, 0, 2)
FLIP = (8 * ROOT[0] + ROOT[1]) ^ (8 * ROOT[2] + 2 * ROOT[3])
F32 = jnp.float32
BF16 = jnp.bfloat16
VMEM = pl.BlockSpec(memory_space=pltpu.VMEM)
SMEM = pl.BlockSpec(memory_space=pltpu.SMEM)
HBM = pl.BlockSpec(memory_space=pltpu.HBM)
UNROLL = 8
SMALL = pltpu.CompilerParams(vmem_limit_bytes=12 << 20)


def swap_groups(v):
    lane = lax.broadcasted_iota(jnp.int32, v[0].shape, 1)
    low = lane < 64
    u = [None] * 4
    for c in (0, 1):
        a, b = v[c], v[c + 2]
        u[c] = jnp.where(low, a, pltpu.roll(b, 64, 1))
        u[c + 2] = jnp.where(low, pltpu.roll(a, 64, 1), b)
    even = (lane & 32) == 0
    out = [None] * 4
    for c in (0, 2):
        a, b = u[c], u[c + 1]
        out[c] = jnp.where(even, a, pltpu.roll(b, 32, 1))
        out[c + 1] = jnp.where(even, pltpu.roll(a, 96, 1), b)
    return out


def project_kernel(
    pair_hbm, gain_hbm, shift_hbm, w_hbm, gain_out_hbm, shift_out_hbm, msg_hbm, gate_hbm,
    pair_ref, w_ref, rows_ref, normed_ref, scr_ref, msg_ref, gate_ref, sem, out_sem,
):
    def pair_copy(t):
        rows = pl.ds(t * 512, 512)
        return pltpu.make_async_copy(pair_hbm.at[rows], pair_ref.at[rows], sem.at[5 + t])

    def gate_copy(t, size):
        rows = pl.ds(t * 512, size)
        return pltpu.make_async_copy(gate_ref.at[rows], gate_hbm.at[rows], out_sem.at[4 + t])

    def msg_copy(t):
        rows = pl.ds(t * 512, 512)
        return pltpu.make_async_copy(msg_ref.at[rows], msg_hbm.at[rows], out_sem.at[t])

    small = [
        pltpu.make_async_copy(ref, rows_ref.at[pl.ds(t * 8, 1)], sem.at[t])
        for t, ref in enumerate((gain_hbm, shift_hbm, gain_out_hbm, shift_out_hbm))
    ]
    w_copy = pltpu.make_async_copy(w_hbm, w_ref, sem.at[4])
    small[0].start()
    small[1].start()
    pair_copy(0).start()
    pair_copy(1).start()
    w_copy.start()
    small[2].start()
    small[3].start()
    small[0].wait()
    small[1].wait()
    gain = rows_ref[0:1, :]
    shift = rows_ref[8:9, :]

    def norm(t, carry):
        pair_copy(t).wait()
        for u in range(4):
            rows = pl.ds(pl.multiple_of(t * 512 + u * 128, 128), 128)
            x = pair_ref[rows, :].astype(F32)
            center = jnp.mean(x, axis=-1, keepdims=True)
            d = x - center
            spread = jnp.mean(d * d, axis=-1, keepdims=True)
            normed_ref[rows, :] = (d * lax.rsqrt(spread + EPSILON) * gain + shift).astype(BF16)
        return carry

    lax.fori_loop(0, 2, norm, 0)
    w_copy.wait()
    wt = jnp.transpose(w_ref[:, :512])
    wg = w_ref[:, 512:640]

    def step(t, carry):
        for u in range(4):
            a = t * 4 + u
            rows = pl.ds(pl.multiple_of(a * 128, 128), 128)
            n = normed_ref[rows, :]
            p = lax.dot_general(wt, n, (((1,), (1,)), ((), ())), preferred_element_type=F32)
            left = jax.nn.sigmoid(p[0:128]) * p[128:256]
            right = jax.nn.sigmoid(p[256:384]) * p[384:512]
            scr_ref[pl.ds(a, 128, stride=16), :] = left
            scr_ref[pl.ds(8 + a, 128, stride=16), :] = right
        return carry

    lax.fori_loop(0, 2, step, 0)

    def pack(t, carry):
        rows = pl.ds(pl.multiple_of(t * 512, 512), 512)
        msg_ref[rows, :] = scr_ref[rows, :].astype(BF16)
        msg_copy(t).start()
        return carry

    lax.fori_loop(0, 4, pack, 0)
    small[2].wait()
    small[3].wait()
    for t in range(2):
        rows = slice(t * 512, (t + 1) * 512)
        gate_ref[rows, :] = jax.nn.sigmoid(
            jnp.dot(normed_ref[rows, :], wg, preferred_element_type=F32)
        )
        if t == 1:
            for k in range(2):
                row = rows_ref[16 + 8 * k : 17 + 8 * k, :]
                gate_ref[1024 + 128 * k : 1152 + 128 * k, :] = jnp.transpose(
                    jnp.broadcast_to(row, (128, 128))
                )
        gate_copy(t, 512 + 256 * t).start()
    for t in range(4):
        msg_copy(t).wait()
    for t in range(2):
        gate_copy(t, 512 + 256 * t).wait()


def spread_kernel(offset, recv_ref, out_ref):
    def step(t, carry):
        for u in range(UNROLL):
            r = t * UNROLL + u
            for g in range(2):
                base = r * 128 + g * 64
                v = []
                for c in range(4):
                    start = pl.multiple_of(base + c * 16, 16)
                    piece = recv_ref[pl.ds(start, 16), :].astype(F32)
                    v.append(piece[offset : offset + 8])
                out_ref[pl.ds(pl.multiple_of(r * 32, 32), 32), g * 128 : (g + 1) * 128] = (
                    jnp.concatenate(swap_groups(v), axis=0).astype(BF16)
                )
        return carry

    lax.fori_loop(0, 16 // UNROLL, step, 0)


def multiply(left_ref, right_ref, mixed_ref):
    mixed_ref[...] = lax.dot_general(
        left_ref[...], right_ref[...], (((0,), (0,)), ((), ())), preferred_element_type=F32
    )


def pieces(mixed_ref, out_ref, row_of):
    def step(t, carry):
        for u in range(4):
            q = t * 4 + u
            for g in range(2):
                v = []
                for b in range(4):
                    start = pl.multiple_of(q * 32 + b * 8, 8)
                    v.append(mixed_ref[pl.ds(start, 8), g * 128 : (g + 1) * 128])
                start = pl.multiple_of(row_of(q) * 64 + g * 32, 32)
                out_ref[pl.ds(start, 32), :] = jnp.concatenate(swap_groups(v), axis=0).astype(BF16)
        return carry

    lax.fori_loop(0, 2, step, 0)


def own_kernel(recv_ref, left_ref, right_ref, out_ref, mixed_ref):
    spread_kernel(8, recv_ref, right_ref)
    multiply(left_ref, right_ref, mixed_ref)
    pieces(mixed_ref, out_ref, lambda q: q)


def other_kernel(core_ref, left_ref, right_ref, own_ref, out_ref, mixed_ref):
    core = core_ref[0]
    multiply(left_ref, right_ref, mixed_ref)
    for q in range(8):
        start = pl.multiple_of(((2 * q + core) ^ FLIP) * 64, 64)
        out_ref[pl.ds(start, 64), :] = own_ref[q * 64 : (q + 1) * 64, :]
    pieces(mixed_ref, out_ref, lambda q: (2 * q + 1 - core) ^ FLIP)


def output_kernel(recv_ref, gate_ref, w_ref, out_ref, scr_ref):
    def total_step(t, sums):
        sums = list(sums)
        for u in range(16):
            rows = pl.ds(pl.multiple_of(t * 256 + u * 16, 16), 16)
            x = recv_ref[rows, :].astype(F32)
            scr_ref[rows, :] = x
            sums[u % 4] = sums[u % 4] + (x[0:8] + x[8:16])
        return tuple(sums)

    zero = jnp.zeros((8, 128), F32)
    sums = lax.fori_loop(0, 4, total_step, (zero,) * 4)
    center = ((sums[0] + sums[1]) + (sums[2] + sums[3])) * (1.0 / 128.0)

    def square_step(t, sums):
        sums = list(sums)
        for u in range(32):
            d = scr_ref[pl.ds(pl.multiple_of(t * 256 + u * 8, 8), 8), :] - center
            sums[u % 4] = sums[u % 4] + d * d
        return tuple(sums)

    sums = lax.fori_loop(0, 4, square_step, (zero,) * 4)
    spread = ((sums[0] + sums[1]) + (sums[2] + sums[3])) * (1.0 / 128.0)
    scale = lax.rsqrt(spread + EPSILON)
    w = w_ref[...]
    gain = gate_ref[1024:1152, :]
    shift = gate_ref[1152:1280, :]
    for s in range(8):
        x = scr_ref[pl.ds(s, 128, stride=8), :]
        x = (x - center[s : s + 1]) * scale[s : s + 1] * gain + shift
        o = lax.dot_general(
            x.astype(BF16), w, (((0,), (0,)), ((), ())), preferred_element_type=F32
        )
        for b in range(4):
            i = b * 8 + s
            rows = slice(i * 32, (i + 1) * 32)
            out_ref[rows, :] = (gate_ref[rows, :] * o[b * 32 : (b + 1) * 32]).astype(BF16)


def chip_groups():
    groups = []
    for core in range(2):
        group = []
        for a, b, c, d in itertools.product(range(2), range(8), range(2), range(4)):
            xh, z, xl, y = a ^ ROOT[0], b ^ ROOT[1], c ^ ROOT[2], d ^ ROOT[3]
            group.append((((xh * 8 + z) * 2 + xl) * 4 + y) * 2 + core)
        groups.append(group)
    return groups


def exchange(x):
    return lax.all_to_all(x, AXES, 0, 0, axis_index_groups=chip_groups(), tiled=True)


def local(pair, norm_in, shift_in, in_weight, norm_out, shift_out, out_weight):
    core = lax.axis_index("core").astype(jnp.int32).reshape(1)
    shape = jax.ShapeDtypeStruct
    msg, gate = pl.pallas_call(
        project_kernel,
        out_shape=(shape((2048, 128), BF16), shape((1280, 128), F32)),
        in_specs=[HBM] * 6,
        out_specs=(HBM,) * 2,
        scratch_shapes=[
            pltpu.VMEM((1024, 128), BF16),
            pltpu.VMEM((128, 640), BF16),
            pltpu.VMEM((32, 128), F32),
            pltpu.VMEM((1024, 128), BF16),
            pltpu.VMEM((2048, 128), F32),
            pltpu.VMEM((2048, 128), BF16),
            pltpu.VMEM((1280, 128), F32),
            pltpu.SemaphoreType.DMA((7,)),
            pltpu.SemaphoreType.DMA((6,)),
        ],
        name="project",
    )(
        pair.reshape(1024, 128),
        norm_in.reshape(1, 128),
        shift_in.reshape(1, 128),
        in_weight,
        norm_out.reshape(1, 128),
        shift_out.reshape(1, 128),
    )
    recv = exchange(msg.reshape(128, 16, 128)).reshape(2048, 128)
    left = pl.pallas_call(
        functools.partial(spread_kernel, 0),
        out_shape=shape((512, 256), BF16),
        in_specs=[VMEM],
        out_specs=VMEM,
        compiler_params=SMALL,
        name="spread",
    )(recv)
    other = lax.ppermute(left, "core", [(0, 1), (1, 0)])
    right, own = pl.pallas_call(
        own_kernel,
        out_shape=(shape((512, 256), BF16), shape((512, 128), BF16)),
        in_specs=[VMEM, VMEM],
        out_specs=(VMEM, VMEM),
        scratch_shapes=[pltpu.VMEM((256, 256), F32)],
        compiler_params=SMALL,
        name="own",
        cost_estimate=pl.CostEstimate(flops=1 << 26, bytes_accessed=1 << 20, transcendentals=0),
    )(recv, left)
    back = pl.pallas_call(
        other_kernel,
        out_shape=shape((1024, 128), BF16),
        in_specs=[SMEM, VMEM, VMEM, VMEM],
        out_specs=VMEM,
        scratch_shapes=[pltpu.VMEM((256, 256), F32)],
        compiler_params=SMALL,
        name="other",
    )(core, other, right, own)
    mixed = exchange(back.reshape(128, 8, 128)).reshape(1024, 128)
    out = pl.pallas_call(
        output_kernel,
        out_shape=shape((1024, 128), BF16),
        in_specs=[VMEM] * 3,
        out_specs=VMEM,
        scratch_shapes=[pltpu.VMEM((1024, 128), F32)],
        compiler_params=SMALL,
        name="output",
    )(mixed, gate, out_weight)
    return out.reshape(pair.shape)


def solution(mesh):
    fine = Mesh(mesh.devices.reshape(2, 8, 2, 4, 2), ("xh", "z", "xl", "y", "core"))
    spec = P(("xh", "z"), ("xl", "y", "core"), None)
    in_specs = (spec, P(), P(), P(), P(), P(), P())
    return jax.shard_map(local, mesh=fine, in_specs=in_specs, out_specs=spec, check_vma=False)
```

```python
import functools
import itertools

import jax
import jax.numpy as jnp
from jax import lax
from jax.experimental import pallas as pl
from jax.experimental.pallas import tpu as pltpu
from jax.sharding import Mesh, PartitionSpec as P

EPSILON = 1e-05
AXES = ("xh", "z", "xl", "y", "core")
ROOT = (1, 4, 0, 2)
FLIP = (8 * ROOT[0] + ROOT[1]) ^ (8 * ROOT[2] + 2 * ROOT[3])
F32 = jnp.float32
BF16 = jnp.bfloat16
VMEM = pl.BlockSpec(memory_space=pltpu.VMEM)
SMEM = pl.BlockSpec(memory_space=pltpu.SMEM)
HBM = pl.BlockSpec(memory_space=pltpu.HBM)
UNROLL = 8
SMALL = pltpu.CompilerParams(vmem_limit_bytes=12 << 20)


def swap_groups(v):
    lane = lax.broadcasted_iota(jnp.int32, v[0].shape, 1)
    low = lane < 64
    u = [None] * 4
    for c in (0, 1):
        a, b = v[c], v[c + 2]
        u[c] = jnp.where(low, a, pltpu.roll(b, 64, 1))
        u[c + 2] = jnp.where(low, pltpu.roll(a, 64, 1), b)
    even = (lane & 32) == 0
    out = [None] * 4
    for c in (0, 2):
        a, b = u[c], u[c + 1]
        out[c] = jnp.where(even, a, pltpu.roll(b, 32, 1))
        out[c + 1] = jnp.where(even, pltpu.roll(a, 96, 1), b)
    return out


def project_kernel(
    pair_hbm, gain_hbm, shift_hbm, w_hbm, gain_out_hbm, shift_out_hbm,
    msg_ref, normed_ref, aux_ref, w_gate_ref,
    pair_ref, w_ref, rows_ref, scr_ref, sem,
):
    def pair_copy(t):
        rows = pl.ds(t * 512, 512)
        return pltpu.make_async_copy(pair_hbm.at[rows], pair_ref.at[rows], sem.at[6 + t])

    small = [
        pltpu.make_async_copy(ref, rows_ref.at[pl.ds(t * 8, 1)], sem.at[t])
        for t, ref in enumerate((gain_hbm, shift_hbm, gain_out_hbm, shift_out_hbm))
    ]
    w_copy = pltpu.make_async_copy(w_hbm.at[:, pl.ds(0, 512)], w_ref, sem.at[4])
    w_gate_copy = pltpu.make_async_copy(w_hbm.at[:, pl.ds(512, 128)], w_gate_ref, sem.at[5])
    small[0].start()
    small[1].start()
    pair_copy(0).start()
    pair_copy(1).start()
    w_copy.start()
    small[2].start()
    small[3].start()
    w_gate_copy.start()
    small[0].wait()
    small[1].wait()
    gain = rows_ref[0:1, :]
    shift = rows_ref[8:9, :]

    def norm(t, carry):
        pair_copy(t).wait()
        for u in range(4):
            rows = pl.ds(pl.multiple_of(t * 512 + u * 128, 128), 128)
            x = pair_ref[rows, :].astype(F32)
            center = jnp.mean(x, axis=-1, keepdims=True)
            d = x - center
            spread = jnp.mean(d * d, axis=-1, keepdims=True)
            normed_ref[rows, :] = (d * lax.rsqrt(spread + EPSILON) * gain + shift).astype(BF16)
        return carry

    lax.fori_loop(0, 2, norm, 0)
    w_copy.wait()
    wt = jnp.transpose(w_ref[...])

    def step(t, carry):
        for u in range(2):
            n = normed_ref[pl.ds(pl.multiple_of(t * 512 + u * 256, 256), 256), :]
            p = lax.dot_general(wt, n, (((1,), (1,)), ((), ())), preferred_element_type=F32)
            left = jax.nn.sigmoid(p[0:128]) * p[128:256]
            right = jax.nn.sigmoid(p[256:384]) * p[384:512]
            for k in range(2):
                a = t * 4 + u * 2 + k
                lanes = slice(k * 128, (k + 1) * 128)
                scr_ref[pl.ds(a, 128, stride=16), :] = left[:, lanes]
                scr_ref[pl.ds(8 + a, 128, stride=16), :] = right[:, lanes]
        return carry

    lax.fori_loop(0, 2, step, 0)

    def pack(t, carry):
        rows = pl.ds(pl.multiple_of(t * 512, 512), 512)
        msg_ref[rows, :] = scr_ref[rows, :].astype(BF16)
        return carry

    lax.fori_loop(0, 4, pack, 0)
    small[2].wait()
    small[3].wait()
    aux_ref[0:1, :] = rows_ref[16:17, :]
    aux_ref[8:9, :] = rows_ref[24:25, :]
    w_gate_copy.wait()


def spread_kernel(offset, recv_ref, out_ref):
    def step(t, carry):
        for u in range(UNROLL):
            r = t * UNROLL + u
            for g in range(2):
                base = r * 128 + g * 64
                v = []
                for c in range(4):
                    start = pl.multiple_of(base + c * 16, 16)
                    piece = recv_ref[pl.ds(start, 16), :].astype(F32)
                    v.append(piece[offset : offset + 8])
                out_ref[pl.ds(pl.multiple_of(r * 32, 32), 32), g * 128 : (g + 1) * 128] = (
                    jnp.concatenate(swap_groups(v), axis=0).astype(BF16)
                )
        return carry

    lax.fori_loop(0, 16 // UNROLL, step, 0)


def multiply(left_ref, right_ref, mixed_ref):
    mixed_ref[...] = lax.dot_general(
        left_ref[...], right_ref[...], (((0,), (0,)), ((), ())), preferred_element_type=F32
    )


def pieces(mixed_ref, out_ref, row_of):
    def step(t, carry):
        for u in range(4):
            q = t * 4 + u
            for g in range(2):
                v = []
                for b in range(4):
                    start = pl.multiple_of(q * 32 + b * 8, 8)
                    v.append(mixed_ref[pl.ds(start, 8), g * 128 : (g + 1) * 128])
                start = pl.multiple_of(row_of(q) * 64 + g * 32, 32)
                out_ref[pl.ds(start, 32), :] = jnp.concatenate(swap_groups(v), axis=0).astype(BF16)
        return carry

    lax.fori_loop(0, 2, step, 0)


def own_kernel(
    recv_ref, left_ref, normed_ref, aux_ref, w_gate_ref, right_ref, out_ref, gate_ref, mixed_ref
):
    spread_kernel(8, recv_ref, right_ref)
    multiply(left_ref, right_ref, mixed_ref)
    gate_ref[0:1024, :] = jax.nn.sigmoid(
        jnp.dot(normed_ref[...], w_gate_ref[...], preferred_element_type=F32)
    )
    pieces(mixed_ref, out_ref, lambda q: q)
    for k in range(2):
        gate_ref[1024 + 128 * k : 1152 + 128 * k, :] = jnp.transpose(
            jnp.broadcast_to(aux_ref[8 * k : 8 * k + 1, :], (128, 128))
        )


def other_kernel(core_ref, left_ref, right_ref, own_ref, out_ref, mixed_ref):
    core = core_ref[0]
    multiply(left_ref, right_ref, mixed_ref)
    for q in range(8):
        start = pl.multiple_of(((2 * q + core) ^ FLIP) * 64, 64)
        out_ref[pl.ds(start, 64), :] = own_ref[q * 64 : (q + 1) * 64, :]
    pieces(mixed_ref, out_ref, lambda q: (2 * q + 1 - core) ^ FLIP)


def output_kernel(recv_ref, gate_ref, w_ref, out_ref, scr_ref):
    def total_step(t, sums):
        sums = list(sums)
        for u in range(16):
            rows = pl.ds(pl.multiple_of(t * 256 + u * 16, 16), 16)
            x = recv_ref[rows, :].astype(F32)
            scr_ref[rows, :] = x
            sums[u % 4] = sums[u % 4] + (x[0:8] + x[8:16])
        return tuple(sums)

    zero = jnp.zeros((8, 128), F32)
    sums = lax.fori_loop(0, 4, total_step, (zero,) * 4)
    center = ((sums[0] + sums[1]) + (sums[2] + sums[3])) * (1.0 / 128.0)

    def square_step(t, sums):
        sums = list(sums)
        for u in range(32):
            d = scr_ref[pl.ds(pl.multiple_of(t * 256 + u * 8, 8), 8), :] - center
            sums[u % 4] = sums[u % 4] + d * d
        return tuple(sums)

    sums = lax.fori_loop(0, 4, square_step, (zero,) * 4)
    spread = ((sums[0] + sums[1]) + (sums[2] + sums[3])) * (1.0 / 128.0)
    scale = lax.rsqrt(spread + EPSILON)
    w = w_ref[...]
    gain = gate_ref[1024:1152, :]
    shift = gate_ref[1152:1280, :]
    for s in range(8):
        x = scr_ref[pl.ds(s, 128, stride=8), :]
        x = (x - center[s : s + 1]) * scale[s : s + 1] * gain + shift
        o = lax.dot_general(
            x.astype(BF16), w, (((0,), (0,)), ((), ())), preferred_element_type=F32
        )
        for b in range(4):
            i = b * 8 + s
            rows = slice(i * 32, (i + 1) * 32)
            out_ref[rows, :] = (gate_ref[rows, :] * o[b * 32 : (b + 1) * 32]).astype(BF16)


def chip_groups():
    groups = []
    for core in range(2):
        group = []
        for a, b, c, d in itertools.product(range(2), range(8), range(2), range(4)):
            xh, z, xl, y = a ^ ROOT[0], b ^ ROOT[1], c ^ ROOT[2], d ^ ROOT[3]
            group.append((((xh * 8 + z) * 2 + xl) * 4 + y) * 2 + core)
        groups.append(group)
    return groups


def exchange(x):
    return lax.all_to_all(x, AXES, 0, 0, axis_index_groups=chip_groups(), tiled=True)


def local(pair, norm_in, shift_in, in_weight, norm_out, shift_out, out_weight):
    core = lax.axis_index("core").astype(jnp.int32).reshape(1)
    shape = jax.ShapeDtypeStruct
    stay = functools.partial(pltpu.with_memory_space_constraint, memory_space=pltpu.HBM)
    msg, normed, aux, w_gate = pl.pallas_call(
        project_kernel,
        out_shape=(
            shape((2048, 128), BF16),
            shape((1024, 128), BF16),
            shape((16, 128), F32),
            shape((128, 128), BF16),
        ),
        in_specs=[HBM] * 6,
        out_specs=(VMEM,) * 4,
        scratch_shapes=[
            pltpu.VMEM((1024, 128), BF16),
            pltpu.VMEM((128, 512), BF16),
            pltpu.VMEM((32, 128), F32),
            pltpu.VMEM((2048, 128), F32),
            pltpu.SemaphoreType.DMA((8,)),
        ],
        compiler_params=SMALL,
        name="project",
    )(
        stay(pair.reshape(1024, 128)),
        stay(norm_in.reshape(1, 128)),
        stay(shift_in.reshape(1, 128)),
        stay(in_weight),
        stay(norm_out.reshape(1, 128)),
        stay(shift_out.reshape(1, 128)),
    )
    recv = exchange(msg.reshape(128, 16, 128)).reshape(2048, 128)
    left = pl.pallas_call(
        functools.partial(spread_kernel, 0),
        out_shape=shape((512, 256), BF16),
        in_specs=[VMEM],
        out_specs=VMEM,
        compiler_params=SMALL,
        name="spread",
    )(recv)
    other = lax.ppermute(left, "core", [(0, 1), (1, 0)])
    right, own, gate = pl.pallas_call(
        own_kernel,
        out_shape=(shape((512, 256), BF16), shape((512, 128), BF16), shape((1280, 128), F32)),
        in_specs=[VMEM] * 5,
        out_specs=(VMEM,) * 3,
        scratch_shapes=[pltpu.VMEM((256, 256), F32)],
        compiler_params=SMALL,
        name="own",
        cost_estimate=pl.CostEstimate(flops=1 << 26, bytes_accessed=1 << 20, transcendentals=0),
    )(recv, left, normed, aux, w_gate)
    back = pl.pallas_call(
        other_kernel,
        out_shape=shape((1024, 128), BF16),
        in_specs=[SMEM, VMEM, VMEM, VMEM],
        out_specs=VMEM,
        scratch_shapes=[pltpu.VMEM((256, 256), F32)],
        compiler_params=SMALL,
        name="other",
    )(core, other, right, own)
    mixed = exchange(back.reshape(128, 8, 128)).reshape(1024, 128)
    out = pl.pallas_call(
        output_kernel,
        out_shape=shape((1024, 128), BF16),
        in_specs=[VMEM] * 3,
        out_specs=VMEM,
        scratch_shapes=[pltpu.VMEM((1024, 128), F32)],
        compiler_params=SMALL,
        name="output",
    )(mixed, gate, out_weight)
    return out.reshape(pair.shape)


def solution(mesh):
    fine = Mesh(mesh.devices.reshape(2, 8, 2, 4, 2), ("xh", "z", "xl", "y", "core"))
    spec = P(("xh", "z"), ("xl", "y", "core"), None)
    in_specs = (spec, P(), P(), P(), P(), P(), P())
    return jax.shard_map(local, mesh=fine, in_specs=in_specs, out_specs=spec, check_vma=False)
```

```python
import functools
import itertools

import jax
import jax.numpy as jnp
from jax import lax
from jax.experimental import pallas as pl
from jax.experimental.pallas import tpu as pltpu
from jax.sharding import Mesh, PartitionSpec as P

EPSILON = 1e-05
AXES = ("xh", "z", "xl", "y", "core")
ROOT = (1, 4, 0, 2)


def hops(p, q):
    def ring(a, b, n):
        return min((a - b) % n, (b - a) % n)

    x = ring(2 * p[0] + p[2], 2 * q[0] + q[2], 4)
    return x + ring(p[1], q[1], 8) + ring(p[3], q[3], 4)


CHIPS = list(itertools.product(range(2), range(8), range(2), range(4)))
CHIPS.sort(key=lambda p: (p != ROOT, -hops(p, ROOT), p))
MEMBER = {p: n for n, p in enumerate(CHIPS)}
F32 = jnp.float32
BF16 = jnp.bfloat16
VMEM = pl.BlockSpec(memory_space=pltpu.VMEM)
SMEM = pl.BlockSpec(memory_space=pltpu.SMEM)
HBM = pl.BlockSpec(memory_space=pltpu.HBM)
SMALL = pltpu.CompilerParams(vmem_limit_bytes=12 << 20)


def swap_groups(v):
    lane = lax.broadcasted_iota(jnp.int32, v[0].shape, 1)
    low = lane < 64
    u = [None] * 4
    for c in (0, 1):
        a, b = v[c], v[c + 2]
        u[c] = jnp.where(low, a, pltpu.roll(b, 64, 1))
        u[c + 2] = jnp.where(low, pltpu.roll(a, 64, 1), b)
    even = (lane & 32) == 0
    out = [None] * 4
    for c in (0, 2):
        a, b = u[c], u[c + 1]
        out[c] = jnp.where(even, a, pltpu.roll(b, 32, 1))
        out[c + 1] = jnp.where(even, pltpu.roll(a, 96, 1), b)
    return out


def project_kernel(
    pair_hbm, gain_hbm, shift_hbm, w_hbm, gain_out_hbm, shift_out_hbm,
    msg_ref, normed_ref, aux_ref, w_gate_ref,
    pair_ref, w_ref, rows_ref, scr_ref, sem,
):
    def pair_copy(t):
        rows = pl.ds(t * 512, 512)
        return pltpu.make_async_copy(pair_hbm.at[rows], pair_ref.at[rows], sem.at[6 + t])

    small = [
        pltpu.make_async_copy(ref, rows_ref.at[pl.ds(t * 8, 1)], sem.at[t])
        for t, ref in enumerate((gain_hbm, shift_hbm, gain_out_hbm, shift_out_hbm))
    ]
    w_copy = pltpu.make_async_copy(w_hbm.at[:, pl.ds(0, 512)], w_ref, sem.at[4])
    w_gate_copy = pltpu.make_async_copy(w_hbm.at[:, pl.ds(512, 128)], w_gate_ref, sem.at[5])
    small[0].start()
    small[1].start()
    pair_copy(0).start()
    pair_copy(1).start()
    w_copy.start()
    small[2].start()
    small[3].start()
    w_gate_copy.start()
    small[0].wait()
    small[1].wait()
    gain = rows_ref[0:1, :]
    shift = rows_ref[8:9, :]

    def norm(t, carry):
        pair_copy(t).wait()
        for u in range(4):
            rows = pl.ds(pl.multiple_of(t * 512 + u * 128, 128), 128)
            x = pair_ref[rows, :].astype(F32)
            center = jnp.mean(x, axis=-1, keepdims=True)
            d = x - center
            spread = jnp.mean(d * d, axis=-1, keepdims=True)
            normed_ref[rows, :] = (d * lax.rsqrt(spread + EPSILON) * gain + shift).astype(BF16)
        return carry

    norm(0, 0)
    w_copy.wait()
    wt = jnp.transpose(w_ref[...])
    norm(1, 0)

    def step(t, carry):
        for u in range(2):
            n = normed_ref[pl.ds(pl.multiple_of(t * 512 + u * 256, 256), 256), :]
            p = lax.dot_general(wt, n, (((1,), (1,)), ((), ())), preferred_element_type=F32)
            left = jax.nn.sigmoid(p[0:128]) * p[128:256]
            right = jax.nn.sigmoid(p[256:384]) * p[384:512]
            for k in range(2):
                a = t * 4 + u * 2 + k
                lanes = slice(k * 128, (k + 1) * 128)
                scr_ref[pl.ds(a, 128, stride=16), :] = left[:, lanes]
                scr_ref[pl.ds(8 + a, 128, stride=16), :] = right[:, lanes]
        return carry

    for t in range(2):
        step(t, 0)

    def pack(t, carry):
        rows = pl.ds(pl.multiple_of(t * 512, 512), 512)
        msg_ref[rows, :] = scr_ref[rows, :].astype(BF16)
        return carry

    lax.fori_loop(0, 4, pack, 0)
    small[2].wait()
    small[3].wait()
    aux_ref[0:1, :] = rows_ref[16:17, :]
    aux_ref[8:9, :] = rows_ref[24:25, :]
    w_gate_copy.wait()


def spread_kernel(offset, recv_ref, out_ref):
    def step(xh, carry):
        for z in range(8):
            for xl in range(2):
                v = []
                for y in range(4):
                    low, high = (MEMBER[(t, z, xl, y)] for t in range(2))
                    start = pl.multiple_of((low + xh * (high - low)) * 16, 16)
                    piece = recv_ref[pl.ds(start, 16), :].astype(F32)
                    v.append(piece[offset : offset + 8])
                start = pl.multiple_of((xh * 8 + z) * 32, 32)
                out_ref[pl.ds(start, 32), xl * 128 : (xl + 1) * 128] = jnp.concatenate(
                    swap_groups(v), axis=0
                ).astype(BF16)
        return carry

    lax.fori_loop(0, 2, step, 0)


def multiply(left_ref, right_ref, mixed_ref):
    mixed_ref[...] = lax.dot_general(
        left_ref[...], right_ref[...], (((0,), (0,)), ((), ())), preferred_element_type=F32
    )


def member(xh, y, core, chip):
    a, b, c, d = (MEMBER[(t, 2 * y + u, *chip)] for t in range(2) for u in range(2))
    return a + xh * (c - a) + core * ((b - a) + xh * (a - b - c + d))


def pieces(mixed_ref, store):
    def step(xl, carry):
        for y in range(4):
            for g in range(2):
                v = []
                for b in range(4):
                    start = pl.multiple_of((xl * 4 + y) * 32 + b * 8, 8)
                    v.append(mixed_ref[pl.ds(start, 8), g * 128 : (g + 1) * 128])
                store(xl, y, g, swap_groups(v))
        return carry

    lax.fori_loop(0, 2, step, 0)


def own_kernel(
    recv_ref, left_ref, normed_ref, aux_ref, w_gate_ref, right_ref, out_ref, gate_ref, mixed_ref
):
    spread_kernel(8, recv_ref, right_ref)
    multiply(left_ref, right_ref, mixed_ref)
    gate_ref[0:1024, :] = jax.nn.sigmoid(
        jnp.dot(normed_ref[...], w_gate_ref[...], preferred_element_type=F32)
    )

    def store(xl, y, g, v):
        start = pl.multiple_of(((xl * 4 + y) * 2 + g) * 32, 32)
        out_ref[pl.ds(start, 32), :] = jnp.concatenate(v, axis=0).astype(BF16)

    pieces(mixed_ref, store)
    for k in range(2):
        gate_ref[1024 + 128 * k : 1152 + 128 * k, :] = jnp.transpose(
            jnp.broadcast_to(aux_ref[8 * k : 8 * k + 1, :], (128, 128))
        )


def other_kernel(core_ref, left_ref, right_ref, own_ref, out_ref, mixed_ref):
    core = core_ref[0]
    multiply(left_ref, right_ref, mixed_ref)

    def store(xl, y, g, v):
        for c in range(4):
            start = pl.multiple_of((xl * 4 + y) * 64 + (g * 4 + c) * 8, 8)
            out_ref[member(xl, y, core, (g, c))] = own_ref[pl.ds(start, 8), :]
            out_ref[member(xl, y, 1 - core, (g, c))] = v[c].astype(BF16)

    pieces(mixed_ref, store)


def output_kernel(recv_ref, gate_ref, w_ref, out_hbm, scr_ref, out_ref, sem):
    def out_copy(half, b):
        rows = pl.ds((b * 8 + half * 4) * 32, 128)
        return pltpu.make_async_copy(out_ref.at[rows], out_hbm.at[rows], sem.at[half * 4 + b])

    def total_step(t, sums):
        sums = list(sums)
        for u in range(16):
            rows = pl.ds(t * 256 + u * 16, 16)
            x = recv_ref[rows, :].astype(F32)
            scr_ref[rows, :] = x
            sums[u % 4] = sums[u % 4] + (x[0:8] + x[8:16])
        return tuple(sums)

    zero = jnp.zeros((8, 128), F32)
    sums = (zero,) * 4
    for t in range(4):
        sums = total_step(t, sums)
    center = ((sums[0] + sums[1]) + (sums[2] + sums[3])) * (1.0 / 128.0)

    def square_step(t, sums):
        sums = list(sums)
        for u in range(32):
            d = scr_ref[pl.ds(t * 256 + u * 8, 8), :] - center
            sums[u % 4] = sums[u % 4] + d * d
        return tuple(sums)

    sums = (zero,) * 4
    for t in range(4):
        sums = square_step(t, sums)
    spread = ((sums[0] + sums[1]) + (sums[2] + sums[3])) * (1.0 / 128.0)
    scale = lax.rsqrt(spread + EPSILON)
    w = w_ref[...]
    gain = gate_ref[1024:1152, :]
    shift = gate_ref[1152:1280, :]
    for s in range(8):
        x = scr_ref[pl.ds(s, 128, stride=8), :]
        x = (x - center[s : s + 1]) * scale[s : s + 1] * gain + shift
        o = lax.dot_general(
            x.astype(BF16), w, (((0,), (0,)), ((), ())), preferred_element_type=F32
        )
        for b in range(4):
            i = b * 8 + s
            rows = slice(i * 32, (i + 1) * 32)
            out_ref[rows, :] = (gate_ref[rows, :] * o[b * 32 : (b + 1) * 32]).astype(BF16)
        if s % 4 == 3:
            for b in range(4):
                out_copy(s // 4, b).start()
    for half in range(2):
        for b in range(4):
            out_copy(half, b).wait()


def chip_groups():
    return [
        [(((xh * 8 + z) * 2 + xl) * 4 + y) * 2 + core for xh, z, xl, y in CHIPS]
        for core in range(2)
    ]


def exchange(x):
    return lax.all_to_all(x, AXES, 0, 0, axis_index_groups=chip_groups(), tiled=True)


def local(pair, norm_in, shift_in, in_weight, norm_out, shift_out, out_weight):
    core = lax.axis_index("core").astype(jnp.int32).reshape(1)
    shape = jax.ShapeDtypeStruct
    stay = functools.partial(pltpu.with_memory_space_constraint, memory_space=pltpu.HBM)
    msg, normed, aux, w_gate = pl.pallas_call(
        project_kernel,
        out_shape=(
            shape((2048, 128), BF16),
            shape((1024, 128), BF16),
            shape((16, 128), F32),
            shape((128, 128), BF16),
        ),
        in_specs=[HBM] * 6,
        out_specs=(VMEM,) * 4,
        scratch_shapes=[
            pltpu.VMEM((1024, 128), BF16),
            pltpu.VMEM((128, 512), BF16),
            pltpu.VMEM((32, 128), F32),
            pltpu.VMEM((2048, 128), F32),
            pltpu.SemaphoreType.DMA((8,)),
        ],
        compiler_params=SMALL,
        name="project",
    )(
        stay(pair.reshape(1024, 128)),
        stay(norm_in.reshape(1, 128)),
        stay(shift_in.reshape(1, 128)),
        stay(in_weight),
        stay(norm_out.reshape(1, 128)),
        stay(shift_out.reshape(1, 128)),
    )
    recv = exchange(msg.reshape(128, 16, 128)).reshape(2048, 128)
    left = pl.pallas_call(
        functools.partial(spread_kernel, 0),
        out_shape=shape((512, 256), BF16),
        in_specs=[VMEM],
        out_specs=VMEM,
        compiler_params=SMALL,
        name="spread",
    )(recv)
    other = lax.ppermute(left, "core", [(0, 1), (1, 0)])
    right, own, gate = pl.pallas_call(
        own_kernel,
        out_shape=(shape((512, 256), BF16), shape((512, 128), BF16), shape((1280, 128), F32)),
        in_specs=[VMEM] * 5,
        out_specs=(VMEM,) * 3,
        scratch_shapes=[pltpu.VMEM((256, 256), F32)],
        compiler_params=SMALL,
        name="own",
        cost_estimate=pl.CostEstimate(flops=1 << 26, bytes_accessed=1 << 20, transcendentals=0),
    )(recv, left, normed, aux, w_gate)
    back = pl.pallas_call(
        other_kernel,
        out_shape=shape((128, 8, 128), BF16),
        in_specs=[SMEM, VMEM, VMEM, VMEM],
        out_specs=VMEM,
        scratch_shapes=[pltpu.VMEM((256, 256), F32)],
        compiler_params=SMALL,
        name="other",
    )(core, other, right, own)
    mixed = exchange(back).reshape(1024, 128)
    out = pl.pallas_call(
        output_kernel,
        out_shape=shape((1024, 128), BF16),
        in_specs=[VMEM] * 3,
        out_specs=HBM,
        scratch_shapes=[
            pltpu.VMEM((1024, 128), F32),
            pltpu.VMEM((1024, 128), BF16),
            pltpu.SemaphoreType.DMA((8,)),
        ],
        compiler_params=SMALL,
        name="output",
    )(mixed, gate, out_weight)
    return out.reshape(pair.shape)


def solution(mesh):
    fine = Mesh(mesh.devices.reshape(2, 8, 2, 4, 2), ("xh", "z", "xl", "y", "core"))
    spec = P(("xh", "z"), ("xl", "y", "core"), None)
    in_specs = (spec, P(), P(), P(), P(), P(), P())
    return jax.shard_map(local, mesh=fine, in_specs=in_specs, out_specs=spec, check_vma=False)
```

```python
import functools
import itertools

import jax
import jax.numpy as jnp
from jax import lax
from jax.experimental import pallas as pl
from jax.experimental.pallas import tpu as pltpu
from jax.sharding import Mesh, PartitionSpec as P

EPSILON = 1e-05
AXES = ("xh", "z", "xl", "y", "core")
ROOT = (1, 5, 0, 2)


def hops(p, q):
    def ring(a, b, n):
        return min((a - b) % n, (b - a) % n)

    x = ring(2 * p[0] + p[2], 2 * q[0] + q[2], 4)
    return x + ring(p[1], q[1], 8) + ring(p[3], q[3], 4)


CHIPS = list(itertools.product(range(2), range(8), range(2), range(4)))
CHIPS.sort(key=lambda p: (p != ROOT, -hops(p, ROOT), p))
MEMBER = {p: n for n, p in enumerate(CHIPS)}
F32 = jnp.float32
BF16 = jnp.bfloat16
VMEM = pl.BlockSpec(memory_space=pltpu.VMEM)
SMEM = pl.BlockSpec(memory_space=pltpu.SMEM)
HBM = pl.BlockSpec(memory_space=pltpu.HBM)
SMALL = pltpu.CompilerParams(vmem_limit_bytes=12 << 20)


def swap_groups(v):
    lane = lax.broadcasted_iota(jnp.int32, v[0].shape, 1)
    low = lane < 64
    u = [None] * 4
    for c in (0, 1):
        a, b = v[c], v[c + 2]
        u[c] = jnp.where(low, a, pltpu.roll(b, 64, 1))
        u[c + 2] = jnp.where(low, pltpu.roll(a, 64, 1), b)
    even = (lane & 32) == 0
    out = [None] * 4
    for c in (0, 2):
        a, b = u[c], u[c + 1]
        out[c] = jnp.where(even, a, pltpu.roll(b, 32, 1))
        out[c + 1] = jnp.where(even, pltpu.roll(a, 96, 1), b)
    return out


def project_kernel(
    pair_hbm, gain_hbm, shift_hbm, w_hbm, gain_out_hbm, shift_out_hbm,
    msg_ref, normed_ref, aux_ref, w_gate_ref,
    pair_ref, w_ref, rows_ref, scr_ref, sem,
):
    def pair_copy(t):
        rows = pl.ds(t * 512, 512)
        return pltpu.make_async_copy(pair_hbm.at[rows], pair_ref.at[rows], sem.at[6 + t])

    small = [
        pltpu.make_async_copy(ref, rows_ref.at[pl.ds(t * 8, 1)], sem.at[t])
        for t, ref in enumerate((gain_hbm, shift_hbm, gain_out_hbm, shift_out_hbm))
    ]
    w_copy = pltpu.make_async_copy(w_hbm.at[:, pl.ds(0, 512)], w_ref, sem.at[4])
    w_gate_copy = pltpu.make_async_copy(w_hbm.at[:, pl.ds(512, 128)], w_gate_ref, sem.at[5])
    small[0].start()
    small[1].start()
    pair_copy(0).start()
    pair_copy(1).start()
    w_copy.start()
    small[2].start()
    small[3].start()
    w_gate_copy.start()
    small[0].wait()
    small[1].wait()
    gain = rows_ref[0:1, :]
    shift = rows_ref[8:9, :]

    def norm(t, carry):
        pair_copy(t).wait()
        for u in range(4):
            rows = pl.ds(pl.multiple_of(t * 512 + u * 128, 128), 128)
            x = pair_ref[rows, :].astype(F32)
            center = jnp.mean(x, axis=-1, keepdims=True)
            d = x - center
            spread = jnp.mean(d * d, axis=-1, keepdims=True)
            normed_ref[rows, :] = (d * lax.rsqrt(spread + EPSILON) * gain + shift).astype(BF16)
        return carry

    norm(0, 0)
    w_copy.wait()
    wt = jnp.transpose(w_ref[...])
    norm(1, 0)

    def step(t, carry):
        for u in range(2):
            n = normed_ref[pl.ds(pl.multiple_of(t * 512 + u * 256, 256), 256), :]
            p = lax.dot_general(wt, n, (((1,), (1,)), ((), ())), preferred_element_type=F32)
            left = jax.nn.sigmoid(p[0:128]) * p[128:256]
            right = jax.nn.sigmoid(p[256:384]) * p[384:512]
            for k in range(2):
                a = t * 4 + u * 2 + k
                lanes = slice(k * 128, (k + 1) * 128)
                scr_ref[pl.ds(a, 128, stride=16), :] = left[:, lanes]
                scr_ref[pl.ds(8 + a, 128, stride=16), :] = right[:, lanes]
        return carry

    for t in range(2):
        step(t, 0)

    def pack(t, carry):
        rows = pl.ds(pl.multiple_of(t * 512, 512), 512)
        msg_ref[rows, :] = scr_ref[rows, :].astype(BF16)
        return carry

    lax.fori_loop(0, 4, pack, 0)
    small[2].wait()
    small[3].wait()
    aux_ref[0:1, :] = rows_ref[16:17, :]
    aux_ref[8:9, :] = rows_ref[24:25, :]
    w_gate_copy.wait()


def spread_kernel(offset, recv_ref, out_ref):
    def step(xh, carry):
        for z in range(8):
            for xl in range(2):
                v = []
                for y in range(4):
                    low, high = (MEMBER[(t, z, xl, y)] for t in range(2))
                    start = pl.multiple_of((low + xh * (high - low)) * 16, 16)
                    piece = recv_ref[pl.ds(start, 16), :].astype(F32)
                    v.append(piece[offset : offset + 8])
                start = pl.multiple_of((xh * 8 + z) * 32, 32)
                out_ref[pl.ds(start, 32), xl * 128 : (xl + 1) * 128] = jnp.concatenate(
                    swap_groups(v), axis=0
                ).astype(BF16)
        return carry

    lax.fori_loop(0, 2, step, 0)


def multiply(left_ref, right_ref, mixed_ref):
    mixed_ref[...] = lax.dot_general(
        left_ref[...], right_ref[...], (((0,), (0,)), ((), ())), preferred_element_type=F32
    )


def member(xh, y, core, chip):
    a, b, c, d = (MEMBER[(t, 2 * y + u, *chip)] for t in range(2) for u in range(2))
    return a + xh * (c - a) + core * ((b - a) + xh * (a - b - c + d))


def pieces(mixed_ref, store, static=False):
    def step(xl, carry):
        for y in range(4):
            for g in range(2):
                v = []
                for b in range(4):
                    start = pl.multiple_of((xl * 4 + y) * 32 + b * 8, 8)
                    v.append(mixed_ref[pl.ds(start, 8), g * 128 : (g + 1) * 128])
                store(xl, y, g, swap_groups(v))
        return carry

    if static:
        for t in range(2):
            step(t, 0)
    else:
        lax.fori_loop(0, 2, step, 0)


def own_kernel(
    recv_ref, left_ref, normed_ref, aux_ref, w_gate_ref, right_ref, out_ref, gate_ref, mixed_ref
):
    spread_kernel(8, recv_ref, right_ref)
    multiply(left_ref, right_ref, mixed_ref)
    gate_ref[0:1024, :] = jax.nn.sigmoid(
        jnp.dot(normed_ref[...], w_gate_ref[...], preferred_element_type=F32)
    )

    def store(xl, y, g, v):
        start = pl.multiple_of(((xl * 4 + y) * 2 + g) * 32, 32)
        out_ref[pl.ds(start, 32), :] = jnp.concatenate(v, axis=0).astype(BF16)

    pieces(mixed_ref, store)
    for k in range(2):
        gate_ref[1024 + 128 * k : 1152 + 128 * k, :] = jnp.transpose(
            jnp.broadcast_to(aux_ref[8 * k : 8 * k + 1, :], (128, 128))
        )


def other_kernel(core_ref, left_ref, right_ref, own_ref, out_ref, mixed_ref):
    core = core_ref[0]
    multiply(left_ref, right_ref, mixed_ref)

    def store(xl, y, g, v):
        for c in range(4):
            start = pl.multiple_of((xl * 4 + y) * 64 + (g * 4 + c) * 8, 8)
            out_ref[member(xl, y, core, (g, c))] = own_ref[pl.ds(start, 8), :]
            out_ref[member(xl, y, 1 - core, (g, c))] = v[c].astype(BF16)

    pieces(mixed_ref, store, True)


def output_kernel(recv_ref, gate_ref, w_ref, out_hbm, scr_ref, out_ref, sem):
    def out_copy(half, b):
        rows = pl.ds((b * 8 + half * 4) * 32, 128)
        return pltpu.make_async_copy(out_ref.at[rows], out_hbm.at[rows], sem.at[half * 4 + b])

    def total_step(t, sums):
        sums = list(sums)
        for u in range(16):
            rows = pl.ds(t * 256 + u * 16, 16)
            x = recv_ref[rows, :].astype(F32)
            scr_ref[rows, :] = x
            sums[u % 4] = sums[u % 4] + (x[0:8] + x[8:16])
        return tuple(sums)

    zero = jnp.zeros((8, 128), F32)
    sums = (zero,) * 4
    for t in range(4):
        sums = total_step(t, sums)
    center = ((sums[0] + sums[1]) + (sums[2] + sums[3])) * (1.0 / 128.0)

    def square_step(t, sums):
        sums = list(sums)
        for u in range(32):
            d = scr_ref[pl.ds(t * 256 + u * 8, 8), :] - center
            sums[u % 4] = sums[u % 4] + d * d
        return tuple(sums)

    sums = (zero,) * 4
    for t in range(4):
        sums = square_step(t, sums)
    spread = ((sums[0] + sums[1]) + (sums[2] + sums[3])) * (1.0 / 128.0)
    scale = lax.rsqrt(spread + EPSILON)
    w = w_ref[...]
    gain = gate_ref[1024:1152, :]
    shift = gate_ref[1152:1280, :]
    for s in range(8):
        x = scr_ref[pl.ds(s, 128, stride=8), :]
        x = (x - center[s : s + 1]) * scale[s : s + 1] * gain + shift
        o = lax.dot_general(
            x.astype(BF16), w, (((0,), (0,)), ((), ())), preferred_element_type=F32
        )
        for b in range(4):
            i = b * 8 + s
            rows = slice(i * 32, (i + 1) * 32)
            out_ref[rows, :] = (gate_ref[rows, :] * o[b * 32 : (b + 1) * 32]).astype(BF16)
        if s % 4 == 3:
            for b in range(4):
                out_copy(s // 4, b).start()
    for half in range(2):
        for b in range(4):
            out_copy(half, b).wait()


def chip_groups():
    return [
        [(((xh * 8 + z) * 2 + xl) * 4 + y) * 2 + core for xh, z, xl, y in CHIPS]
        for core in range(2)
    ]


def exchange(x):
    return lax.all_to_all(x, AXES, 0, 0, axis_index_groups=chip_groups(), tiled=True)


def local(pair, norm_in, shift_in, in_weight, norm_out, shift_out, out_weight):
    core = lax.axis_index("core").astype(jnp.int32).reshape(1)
    shape = jax.ShapeDtypeStruct
    stay = functools.partial(pltpu.with_memory_space_constraint, memory_space=pltpu.HBM)
    msg, normed, aux, w_gate = pl.pallas_call(
        project_kernel,
        out_shape=(
            shape((2048, 128), BF16),
            shape((1024, 128), BF16),
            shape((16, 128), F32),
            shape((128, 128), BF16),
        ),
        in_specs=[HBM] * 6,
        out_specs=(VMEM,) * 4,
        scratch_shapes=[
            pltpu.VMEM((1024, 128), BF16),
            pltpu.VMEM((128, 512), BF16),
            pltpu.VMEM((32, 128), F32),
            pltpu.VMEM((2048, 128), F32),
            pltpu.SemaphoreType.DMA((8,)),
        ],
        compiler_params=SMALL,
        name="project",
    )(
        stay(pair.reshape(1024, 128)),
        stay(norm_in.reshape(1, 128)),
        stay(shift_in.reshape(1, 128)),
        stay(in_weight),
        stay(norm_out.reshape(1, 128)),
        stay(shift_out.reshape(1, 128)),
    )
    recv = exchange(msg.reshape(128, 16, 128)).reshape(2048, 128)
    left = pl.pallas_call(
        functools.partial(spread_kernel, 0),
        out_shape=shape((512, 256), BF16),
        in_specs=[VMEM],
        out_specs=VMEM,
        compiler_params=SMALL,
        name="spread",
    )(recv)
    other = lax.ppermute(left, "core", [(0, 1), (1, 0)])
    right, own, gate = pl.pallas_call(
        own_kernel,
        out_shape=(shape((512, 256), BF16), shape((512, 128), BF16), shape((1280, 128), F32)),
        in_specs=[VMEM] * 5,
        out_specs=(VMEM,) * 3,
        scratch_shapes=[pltpu.VMEM((256, 256), F32)],
        compiler_params=SMALL,
        name="own",
        cost_estimate=pl.CostEstimate(flops=1 << 26, bytes_accessed=1 << 20, transcendentals=0),
    )(recv, left, normed, aux, w_gate)
    back = pl.pallas_call(
        other_kernel,
        out_shape=shape((128, 8, 128), BF16),
        in_specs=[SMEM, VMEM, VMEM, VMEM],
        out_specs=VMEM,
        scratch_shapes=[pltpu.VMEM((256, 256), F32)],
        compiler_params=SMALL,
        name="other",
    )(core, other, right, own)
    mixed = exchange(back).reshape(1024, 128)
    out = pl.pallas_call(
        output_kernel,
        out_shape=shape((1024, 128), BF16),
        in_specs=[VMEM] * 3,
        out_specs=HBM,
        scratch_shapes=[
            pltpu.VMEM((1024, 128), F32),
            pltpu.VMEM((1024, 128), BF16),
            pltpu.SemaphoreType.DMA((8,)),
        ],
        compiler_params=SMALL,
        name="output",
    )(mixed, gate, out_weight)
    return out.reshape(pair.shape)


def solution(mesh):
    fine = Mesh(mesh.devices.reshape(2, 8, 2, 4, 2), ("xh", "z", "xl", "y", "core"))
    spec = P(("xh", "z"), ("xl", "y", "core"), None)
    in_specs = (spec, P(), P(), P(), P(), P(), P())
    return jax.shard_map(local, mesh=fine, in_specs=in_specs, out_specs=spec, check_vma=False)
```

```python
import functools
import itertools

import jax
import jax.numpy as jnp
from jax import lax
from jax.experimental import pallas as pl
from jax.experimental.pallas import tpu as pltpu
from jax.sharding import Mesh, PartitionSpec as P

EPSILON = 1e-05
AXES = ("xh", "z", "xl", "y", "core")
ROOT = (1, 5, 0, 2)


def hops(p, q):
    def ring(a, b, n):
        return min((a - b) % n, (b - a) % n)

    x = ring(2 * p[0] + p[2], 2 * q[0] + q[2], 4)
    return x + ring(p[1], q[1], 8) + ring(p[3], q[3], 4)


CHIPS = list(itertools.product(range(2), range(8), range(2), range(4)))
CHIPS.sort(key=lambda p: (p != ROOT, -hops(p, ROOT), p))
MEMBER = {p: n for n, p in enumerate(CHIPS)}
F32 = jnp.float32
BF16 = jnp.bfloat16
VMEM = pl.BlockSpec(memory_space=pltpu.VMEM)
SMEM = pl.BlockSpec(memory_space=pltpu.SMEM)
HBM = pl.BlockSpec(memory_space=pltpu.HBM)
SMALL = pltpu.CompilerParams(vmem_limit_bytes=12 << 20)


def swap_groups(v):
    lane = lax.broadcasted_iota(jnp.int32, v[0].shape, 1)
    low = lane < 64
    u = [None] * 4
    for c in (0, 1):
        a, b = v[c], v[c + 2]
        u[c] = jnp.where(low, a, pltpu.roll(b, 64, 1))
        u[c + 2] = jnp.where(low, pltpu.roll(a, 64, 1), b)
    even = (lane & 32) == 0
    out = [None] * 4
    for c in (0, 2):
        a, b = u[c], u[c + 1]
        out[c] = jnp.where(even, a, pltpu.roll(b, 32, 1))
        out[c + 1] = jnp.where(even, pltpu.roll(a, 96, 1), b)
    return out


def project_kernel(
    pair_hbm, gain_hbm, shift_hbm, w_hbm, msg_ref, normed_ref,
    pair_ref, w_ref, rows_ref, scr_ref, sem,
):
    def pair_copy(t):
        rows = pl.ds(t * 512, 512)
        return pltpu.make_async_copy(pair_hbm.at[rows], pair_ref.at[rows], sem.at[3 + t])

    small = [
        pltpu.make_async_copy(ref, rows_ref.at[pl.ds(t * 8, 1)], sem.at[t])
        for t, ref in enumerate((gain_hbm, shift_hbm))
    ]
    w_copy = pltpu.make_async_copy(w_hbm.at[:, pl.ds(0, 512)], w_ref, sem.at[2])
    pair_copy(0).start()
    small[0].start()
    small[1].start()
    w_copy.start()
    pair_copy(1).start()
    small[0].wait()
    small[1].wait()
    gain = rows_ref[0:1, :]
    shift = rows_ref[8:9, :]

    def norm(t, carry):
        pair_copy(t).wait()
        for u in range(4):
            rows = pl.ds(pl.multiple_of(t * 512 + u * 128, 128), 128)
            x = pair_ref[rows, :].astype(F32)
            center = jnp.mean(x, axis=-1, keepdims=True)
            d = x - center
            spread = jnp.mean(d * d, axis=-1, keepdims=True)
            normed_ref[rows, :] = (d * lax.rsqrt(spread + EPSILON) * gain + shift).astype(BF16)
        return carry

    norm(0, 0)
    w_copy.wait()
    wt = jnp.transpose(w_ref[...])
    norm(1, 0)

    def step(t, carry):
        for u in range(2):
            n = normed_ref[pl.ds(pl.multiple_of(t * 512 + u * 256, 256), 256), :]
            p = lax.dot_general(wt, n, (((1,), (1,)), ((), ())), preferred_element_type=F32)
            left = jax.nn.sigmoid(p[0:128]) * p[128:256]
            right = jax.nn.sigmoid(p[256:384]) * p[384:512]
            for k in range(2):
                a = t * 4 + u * 2 + k
                lanes = slice(k * 128, (k + 1) * 128)
                scr_ref[pl.ds(a, 128, stride=16), :] = left[:, lanes]
                scr_ref[pl.ds(8 + a, 128, stride=16), :] = right[:, lanes]
        return carry

    for t in range(2):
        step(t, 0)

    def pack(t, carry):
        rows = pl.ds(pl.multiple_of(t * 512, 512), 512)
        msg_ref[rows, :] = scr_ref[rows, :].astype(BF16)
        return carry

    lax.fori_loop(0, 4, pack, 0)


def spread_kernel(offset, recv_ref, out_ref):
    def step(xh, carry):
        for z in range(8):
            for xl in range(2):
                v = []
                for y in range(4):
                    low, high = (MEMBER[(t, z, xl, y)] for t in range(2))
                    start = pl.multiple_of((low + xh * (high - low)) * 16, 16)
                    piece = recv_ref[pl.ds(start, 16), :].astype(F32)
                    v.append(piece[offset : offset + 8])
                start = pl.multiple_of((xh * 8 + z) * 32, 32)
                out_ref[pl.ds(start, 32), xl * 128 : (xl + 1) * 128] = jnp.concatenate(
                    swap_groups(v), axis=0
                ).astype(BF16)
        return carry

    lax.fori_loop(0, 2, step, 0)


def multiply(left_ref, right_ref, mixed_ref):
    mixed_ref[...] = lax.dot_general(
        left_ref[...], right_ref[...], (((0,), (0,)), ((), ())), preferred_element_type=F32
    )


def member(xh, y, core, chip):
    a, b, c, d = (MEMBER[(t, 2 * y + u, *chip)] for t in range(2) for u in range(2))
    return a + xh * (c - a) + core * ((b - a) + xh * (a - b - c + d))


def pieces(mixed_ref, store, static=False):
    def step(xl, carry):
        for y in range(4):
            for g in range(2):
                v = []
                for b in range(4):
                    start = pl.multiple_of((xl * 4 + y) * 32 + b * 8, 8)
                    v.append(mixed_ref[pl.ds(start, 8), g * 128 : (g + 1) * 128])
                store(xl, y, g, swap_groups(v))
        return carry

    if static:
        for t in range(2):
            step(t, 0)
    else:
        lax.fori_loop(0, 2, step, 0)


def own_kernel(
    recv_ref, left_ref, normed_ref, gain_hbm, shift_hbm, w_hbm,
    right_ref, out_ref, gate_ref,
    mixed_ref, rows_ref, w_gate_ref, sem,
):
    copies = [
        pltpu.make_async_copy(w_hbm.at[:, pl.ds(512, 128)], w_gate_ref, sem.at[0]),
        pltpu.make_async_copy(gain_hbm, rows_ref.at[pl.ds(0, 1)], sem.at[1]),
        pltpu.make_async_copy(shift_hbm, rows_ref.at[pl.ds(8, 1)], sem.at[2]),
    ]
    for copy in copies:
        copy.start()
    spread_kernel(8, recv_ref, right_ref)
    multiply(left_ref, right_ref, mixed_ref)

    def store(xl, y, g, v):
        start = pl.multiple_of(((xl * 4 + y) * 2 + g) * 32, 32)
        out_ref[pl.ds(start, 32), :] = jnp.concatenate(v, axis=0).astype(BF16)

    pieces(mixed_ref, store, True)
    for copy in copies:
        copy.wait()
    gate_ref[0:1024, :] = jax.nn.sigmoid(
        jnp.dot(normed_ref[...], w_gate_ref[...], preferred_element_type=F32)
    )
    for k in range(2):
        gate_ref[1024 + 128 * k : 1152 + 128 * k, :] = jnp.transpose(
            jnp.broadcast_to(rows_ref[8 * k : 8 * k + 1, :], (128, 128))
        )


def other_kernel(core_ref, left_ref, right_ref, own_ref, out_ref, mixed_ref):
    core = core_ref[0]
    multiply(left_ref, right_ref, mixed_ref)

    def store(xl, y, g, v):
        for c in range(4):
            start = pl.multiple_of((xl * 4 + y) * 64 + (g * 4 + c) * 8, 8)
            out_ref[member(xl, y, core, (g, c))] = own_ref[pl.ds(start, 8), :]
            out_ref[member(xl, y, 1 - core, (g, c))] = v[c].astype(BF16)

    pieces(mixed_ref, store, True)


def output_kernel(recv_ref, gate_ref, w_ref, out_hbm, scr_ref, out_ref, sem):
    def out_copy(half, b):
        rows = pl.ds((b * 8 + half * 4) * 32, 128)
        return pltpu.make_async_copy(out_ref.at[rows], out_hbm.at[rows], sem.at[half * 4 + b])

    def total_step(t, sums):
        sums = list(sums)
        for u in range(16):
            rows = pl.ds(t * 256 + u * 16, 16)
            x = recv_ref[rows, :].astype(F32)
            scr_ref[rows, :] = x
            sums[u % 4] = sums[u % 4] + (x[0:8] + x[8:16])
        return tuple(sums)

    zero = jnp.zeros((8, 128), F32)
    sums = (zero,) * 4
    for t in range(4):
        sums = total_step(t, sums)
    center = ((sums[0] + sums[1]) + (sums[2] + sums[3])) * (1.0 / 128.0)

    def square_step(t, sums):
        sums = list(sums)
        for u in range(32):
            d = scr_ref[pl.ds(t * 256 + u * 8, 8), :] - center
            sums[u % 4] = sums[u % 4] + d * d
        return tuple(sums)

    sums = (zero,) * 4
    for t in range(4):
        sums = square_step(t, sums)
    spread = ((sums[0] + sums[1]) + (sums[2] + sums[3])) * (1.0 / 128.0)
    scale = lax.rsqrt(spread + EPSILON)
    w = w_ref[...]
    gain = gate_ref[1024:1152, :]
    shift = gate_ref[1152:1280, :]
    for s in range(8):
        x = scr_ref[pl.ds(s, 128, stride=8), :]
        x = (x - center[s : s + 1]) * scale[s : s + 1] * gain + shift
        o = lax.dot_general(
            x.astype(BF16), w, (((0,), (0,)), ((), ())), preferred_element_type=F32
        )
        for b in range(4):
            i = b * 8 + s
            rows = slice(i * 32, (i + 1) * 32)
            out_ref[rows, :] = (gate_ref[rows, :] * o[b * 32 : (b + 1) * 32]).astype(BF16)
        if s % 4 == 3:
            for b in range(4):
                out_copy(s // 4, b).start()
    for half in range(2):
        for b in range(4):
            out_copy(half, b).wait()


def chip_groups():
    return [
        [(((xh * 8 + z) * 2 + xl) * 4 + y) * 2 + core for xh, z, xl, y in CHIPS]
        for core in range(2)
    ]


def exchange(x):
    return lax.all_to_all(x, AXES, 0, 0, axis_index_groups=chip_groups(), tiled=True)


def local(pair, norm_in, shift_in, in_weight, norm_out, shift_out, out_weight):
    core = lax.axis_index("core").astype(jnp.int32).reshape(1)
    shape = jax.ShapeDtypeStruct
    stay = functools.partial(pltpu.with_memory_space_constraint, memory_space=pltpu.HBM)
    msg, normed = pl.pallas_call(
        project_kernel,
        out_shape=(shape((2048, 128), BF16), shape((1024, 128), BF16)),
        in_specs=[HBM] * 4,
        out_specs=(VMEM,) * 2,
        scratch_shapes=[
            pltpu.VMEM((1024, 128), BF16),
            pltpu.VMEM((128, 512), BF16),
            pltpu.VMEM((16, 128), F32),
            pltpu.VMEM((2048, 128), F32),
            pltpu.SemaphoreType.DMA((5,)),
        ],
        compiler_params=SMALL,
        name="project",
    )(
        stay(pair.reshape(1024, 128)),
        stay(norm_in.reshape(1, 128)),
        stay(shift_in.reshape(1, 128)),
        stay(in_weight),
    )
    recv = exchange(msg.reshape(128, 16, 128)).reshape(2048, 128)
    left = pl.pallas_call(
        functools.partial(spread_kernel, 0),
        out_shape=shape((512, 256), BF16),
        in_specs=[VMEM],
        out_specs=VMEM,
        compiler_params=SMALL,
        name="spread",
    )(recv)
    other = lax.ppermute(left, "core", [(0, 1), (1, 0)])
    right, own, gate = pl.pallas_call(
        own_kernel,
        out_shape=(shape((512, 256), BF16), shape((512, 128), BF16), shape((1280, 128), F32)),
        in_specs=[VMEM] * 3 + [HBM] * 3,
        out_specs=(VMEM,) * 3,
        scratch_shapes=[
            pltpu.VMEM((256, 256), F32),
            pltpu.VMEM((16, 128), F32),
            pltpu.VMEM((128, 128), BF16),
            pltpu.SemaphoreType.DMA((3,)),
        ],
        compiler_params=SMALL,
        name="own",
        cost_estimate=pl.CostEstimate(flops=1 << 26, bytes_accessed=1 << 20, transcendentals=0),
    )(
        recv,
        left,
        normed,
        stay(norm_out.reshape(1, 128)),
        stay(shift_out.reshape(1, 128)),
        stay(in_weight),
    )
    back = pl.pallas_call(
        other_kernel,
        out_shape=shape((128, 8, 128), BF16),
        in_specs=[SMEM, VMEM, VMEM, VMEM],
        out_specs=VMEM,
        scratch_shapes=[pltpu.VMEM((256, 256), F32)],
        compiler_params=SMALL,
        name="other",
    )(core, other, right, own)
    mixed = exchange(back).reshape(1024, 128)
    out = pl.pallas_call(
        output_kernel,
        out_shape=shape((1024, 128), BF16),
        in_specs=[VMEM] * 3,
        out_specs=HBM,
        scratch_shapes=[
            pltpu.VMEM((1024, 128), F32),
            pltpu.VMEM((1024, 128), BF16),
            pltpu.SemaphoreType.DMA((8,)),
        ],
        compiler_params=SMALL,
        name="output",
    )(mixed, gate, out_weight)
    return out.reshape(pair.shape)


def solution(mesh):
    fine = Mesh(mesh.devices.reshape(2, 8, 2, 4, 2), ("xh", "z", "xl", "y", "core"))
    spec = P(("xh", "z"), ("xl", "y", "core"), None)
    in_specs = (spec, P(), P(), P(), P(), P(), P())
    return jax.shard_map(local, mesh=fine, in_specs=in_specs, out_specs=spec, check_vma=False)
```

```python
import functools
import itertools

import jax
import jax.numpy as jnp
from jax import lax
from jax.experimental import pallas as pl
from jax.experimental.pallas import tpu as pltpu
from jax.sharding import Mesh, PartitionSpec as P

EPSILON = 1e-05
AXES = ("xh", "z", "xl", "y", "core")
ROOT = (1, 5, 0, 2)


def hops(p, q):
    def ring(a, b, n):
        return min((a - b) % n, (b - a) % n)

    x = ring(2 * p[0] + p[2], 2 * q[0] + q[2], 4)
    return x + ring(p[1], q[1], 8) + ring(p[3], q[3], 4)


CHIPS = list(itertools.product(range(2), range(8), range(2), range(4)))
CHIPS.sort(key=lambda p: (p != ROOT, -hops(p, ROOT), p))
MEMBER = {p: n for n, p in enumerate(CHIPS)}
F32 = jnp.float32
BF16 = jnp.bfloat16
VMEM = pl.BlockSpec(memory_space=pltpu.VMEM)
SMEM = pl.BlockSpec(memory_space=pltpu.SMEM)
HBM = pl.BlockSpec(memory_space=pltpu.HBM)
SMALL = pltpu.CompilerParams(vmem_limit_bytes=12 << 20)


def swap_groups(v):
    lane = lax.broadcasted_iota(jnp.int32, v[0].shape, 1)
    low = lane < 64
    u = [None] * 4
    for c in (0, 1):
        a, b = v[c], v[c + 2]
        u[c] = jnp.where(low, a, pltpu.roll(b, 64, 1))
        u[c + 2] = jnp.where(low, pltpu.roll(a, 64, 1), b)
    even = (lane & 32) == 0
    out = [None] * 4
    for c in (0, 2):
        a, b = u[c], u[c + 1]
        out[c] = jnp.where(even, a, pltpu.roll(b, 32, 1))
        out[c + 1] = jnp.where(even, pltpu.roll(a, 96, 1), b)
    return out


def project_kernel(
    pair_hbm, gain_hbm, shift_hbm, w_hbm, gain_out_hbm, shift_out_hbm,
    msg_ref, normed_ref, aux_ref, w_gate_ref,
    pair_ref, w_ref, rows_ref, scr_ref, sem,
):
    def pair_copy(t):
        rows = pl.ds(t * 512, 512)
        return pltpu.make_async_copy(pair_hbm.at[rows], pair_ref.at[rows], sem.at[6 + t])

    small = [
        pltpu.make_async_copy(ref, rows_ref.at[pl.ds(t * 8, 1)], sem.at[t])
        for t, ref in enumerate((gain_hbm, shift_hbm, gain_out_hbm, shift_out_hbm))
    ]
    w_copy = pltpu.make_async_copy(w_hbm.at[:, pl.ds(0, 512)], w_ref, sem.at[4])
    w_gate_copy = pltpu.make_async_copy(w_hbm.at[:, pl.ds(512, 128)], w_gate_ref, sem.at[5])
    pair_copy(0).start()
    small[0].start()
    small[1].start()
    w_copy.start()
    pair_copy(1).start()
    small[2].start()
    small[3].start()
    w_gate_copy.start()
    small[0].wait()
    small[1].wait()
    gain = rows_ref[0:1, :]
    shift = rows_ref[8:9, :]

    def norm(t, carry):
        pair_copy(t).wait()
        for u in range(4):
            rows = pl.ds(pl.multiple_of(t * 512 + u * 128, 128), 128)
            x = pair_ref[rows, :].astype(F32)
            center = jnp.mean(x, axis=-1, keepdims=True)
            d = x - center
            spread = jnp.mean(d * d, axis=-1, keepdims=True)
            normed_ref[rows, :] = (d * lax.rsqrt(spread + EPSILON) * gain + shift).astype(BF16)
        return carry

    norm(0, 0)
    w_copy.wait()
    wt = jnp.transpose(w_ref[...])
    norm(1, 0)

    def step(t, carry):
        for u in range(2):
            n = normed_ref[pl.ds(pl.multiple_of(t * 512 + u * 256, 256), 256), :]
            p = lax.dot_general(wt, n, (((1,), (1,)), ((), ())), preferred_element_type=F32)
            left = jax.nn.sigmoid(p[0:128]) * p[128:256]
            right = jax.nn.sigmoid(p[256:384]) * p[384:512]
            for k in range(2):
                a = t * 4 + u * 2 + k
                lanes = slice(k * 128, (k + 1) * 128)
                scr_ref[pl.ds(a, 128, stride=16), :] = left[:, lanes]
                scr_ref[pl.ds(8 + a, 128, stride=16), :] = right[:, lanes]
        return carry

    for t in range(2):
        step(t, 0)

    def pack(t, carry):
        rows = pl.ds(pl.multiple_of(t * 512, 512), 512)
        msg_ref[rows, :] = scr_ref[rows, :].astype(BF16)
        return carry

    lax.fori_loop(0, 4, pack, 0)
    small[2].wait()
    small[3].wait()
    aux_ref[0:1, :] = rows_ref[16:17, :]
    aux_ref[8:9, :] = rows_ref[24:25, :]
    w_gate_copy.wait()


def spread_kernel(offset, recv_ref, out_ref):
    def step(xh, carry):
        for z in range(8):
            for xl in range(2):
                v = []
                for y in range(4):
                    low, high = (MEMBER[(t, z, xl, y)] for t in range(2))
                    start = pl.multiple_of((low + xh * (high - low)) * 16, 16)
                    piece = recv_ref[pl.ds(start, 16), :].astype(F32)
                    v.append(piece[offset : offset + 8])
                start = pl.multiple_of((xh * 8 + z) * 32, 32)
                out_ref[pl.ds(start, 32), xl * 128 : (xl + 1) * 128] = jnp.concatenate(
                    swap_groups(v), axis=0
                ).astype(BF16)
        return carry

    lax.fori_loop(0, 2, step, 0)


def multiply(left_ref, right_ref, mixed_ref):
    mixed_ref[...] = lax.dot_general(
        left_ref[...], right_ref[...], (((0,), (0,)), ((), ())), preferred_element_type=F32
    )


def member(xh, y, core, chip):
    a, b, c, d = (MEMBER[(t, 2 * y + u, *chip)] for t in range(2) for u in range(2))
    return a + xh * (c - a) + core * ((b - a) + xh * (a - b - c + d))


def pieces(mixed_ref, store, static=False):
    def step(xl, carry):
        for y in range(4):
            for g in range(2):
                v = []
                for b in range(4):
                    start = pl.multiple_of((xl * 4 + y) * 32 + b * 8, 8)
                    v.append(mixed_ref[pl.ds(start, 8), g * 128 : (g + 1) * 128])
                store(xl, y, g, swap_groups(v))
        return carry

    if static:
        for t in range(2):
            step(t, 0)
    else:
        lax.fori_loop(0, 2, step, 0)


def own_kernel(
    recv_ref, left_ref, normed_ref, aux_ref, w_gate_ref, right_ref, out_ref, gate_ref, mixed_ref
):
    spread_kernel(8, recv_ref, right_ref)
    multiply(left_ref, right_ref, mixed_ref)
    gate_ref[0:1024, :] = jax.nn.sigmoid(
        jnp.dot(normed_ref[...], w_gate_ref[...], preferred_element_type=F32)
    )

    def store(xl, y, g, v):
        start = pl.multiple_of(((xl * 4 + y) * 2 + g) * 32, 32)
        out_ref[pl.ds(start, 32), :] = jnp.concatenate(v, axis=0).astype(BF16)

    pieces(mixed_ref, store, True)
    for k in range(2):
        gate_ref[1024 + 128 * k : 1152 + 128 * k, :] = jnp.transpose(
            jnp.broadcast_to(aux_ref[8 * k : 8 * k + 1, :], (128, 128))
        )


def other_kernel(core_ref, left_ref, right_ref, own_ref, out_ref, mixed_ref):
    core = core_ref[0]
    multiply(left_ref, right_ref, mixed_ref)

    def store(xl, y, g, v):
        for c in range(4):
            start = pl.multiple_of((xl * 4 + y) * 64 + (g * 4 + c) * 8, 8)
            out_ref[member(xl, y, core, (g, c))] = own_ref[pl.ds(start, 8), :]
            out_ref[member(xl, y, 1 - core, (g, c))] = v[c].astype(BF16)

    pieces(mixed_ref, store, True)


def output_kernel(recv_ref, gate_ref, w_ref, out_hbm, scr_ref, out_ref, sem):
    def out_copy(half, b):
        rows = pl.ds((b * 8 + half * 4) * 32, 128)
        return pltpu.make_async_copy(out_ref.at[rows], out_hbm.at[rows], sem.at[half * 4 + b])

    def total_step(t, sums):
        sums = list(sums)
        for u in range(16):
            rows = pl.ds(t * 256 + u * 16, 16)
            x = recv_ref[rows, :].astype(F32)
            scr_ref[rows, :] = x
            sums[u % 4] = sums[u % 4] + (x[0:8] + x[8:16])
        return tuple(sums)

    zero = jnp.zeros((8, 128), F32)
    sums = (zero,) * 4
    for t in range(4):
        sums = total_step(t, sums)
    center = ((sums[0] + sums[1]) + (sums[2] + sums[3])) * (1.0 / 128.0)

    def square_step(t, sums):
        sums = list(sums)
        for u in range(32):
            d = scr_ref[pl.ds(t * 256 + u * 8, 8), :] - center
            sums[u % 4] = sums[u % 4] + d * d
        return tuple(sums)

    sums = (zero,) * 4
    for t in range(4):
        sums = square_step(t, sums)
    spread = ((sums[0] + sums[1]) + (sums[2] + sums[3])) * (1.0 / 128.0)
    scale = lax.rsqrt(spread + EPSILON)
    w = w_ref[...]
    gain = gate_ref[1024:1152, :]
    shift = gate_ref[1152:1280, :]
    for s in range(8):
        x = scr_ref[pl.ds(s, 128, stride=8), :]
        x = (x - center[s : s + 1]) * scale[s : s + 1] * gain + shift
        o = lax.dot_general(
            x.astype(BF16), w, (((0,), (0,)), ((), ())), preferred_element_type=F32
        )
        for b in range(4):
            i = b * 8 + s
            rows = slice(i * 32, (i + 1) * 32)
            out_ref[rows, :] = (gate_ref[rows, :] * o[b * 32 : (b + 1) * 32]).astype(BF16)
        if s % 4 == 3:
            for b in range(4):
                out_copy(s // 4, b).start()
    for half in range(2):
        for b in range(4):
            out_copy(half, b).wait()


def chip_groups():
    return [
        [(((xh * 8 + z) * 2 + xl) * 4 + y) * 2 + core for xh, z, xl, y in CHIPS]
        for core in range(2)
    ]


def exchange(x):
    return lax.all_to_all(x, AXES, 0, 0, axis_index_groups=chip_groups(), tiled=True)


def local(pair, norm_in, shift_in, in_weight, norm_out, shift_out, out_weight):
    core = lax.axis_index("core").astype(jnp.int32).reshape(1)
    shape = jax.ShapeDtypeStruct
    stay = functools.partial(pltpu.with_memory_space_constraint, memory_space=pltpu.HBM)
    msg, normed, aux, w_gate = pl.pallas_call(
        project_kernel,
        out_shape=(
            shape((2048, 128), BF16),
            shape((1024, 128), BF16),
            shape((16, 128), F32),
            shape((128, 128), BF16),
        ),
        in_specs=[HBM] * 6,
        out_specs=(VMEM,) * 4,
        scratch_shapes=[
            pltpu.VMEM((1024, 128), BF16),
            pltpu.VMEM((128, 512), BF16),
            pltpu.VMEM((32, 128), F32),
            pltpu.VMEM((2048, 128), F32),
            pltpu.SemaphoreType.DMA((8,)),
        ],
        compiler_params=SMALL,
        name="project",
    )(
        stay(pair.reshape(1024, 128)),
        stay(norm_in.reshape(1, 128)),
        stay(shift_in.reshape(1, 128)),
        stay(in_weight),
        stay(norm_out.reshape(1, 128)),
        stay(shift_out.reshape(1, 128)),
    )
    recv = exchange(msg.reshape(128, 16, 128)).reshape(2048, 128)
    left = pl.pallas_call(
        functools.partial(spread_kernel, 0),
        out_shape=shape((512, 256), BF16),
        in_specs=[VMEM],
        out_specs=VMEM,
        compiler_params=SMALL,
        name="spread",
    )(recv)
    other = lax.ppermute(left, "core", [(0, 1), (1, 0)])
    right, own, gate = pl.pallas_call(
        own_kernel,
        out_shape=(shape((512, 256), BF16), shape((512, 128), BF16), shape((1280, 128), F32)),
        in_specs=[VMEM] * 5,
        out_specs=(VMEM,) * 3,
        scratch_shapes=[pltpu.VMEM((256, 256), F32)],
        compiler_params=SMALL,
        name="own",
        cost_estimate=pl.CostEstimate(flops=1 << 26, bytes_accessed=1 << 20, transcendentals=0),
    )(recv, left, normed, aux, w_gate)
    back = pl.pallas_call(
        other_kernel,
        out_shape=shape((128, 8, 128), BF16),
        in_specs=[SMEM, VMEM, VMEM, VMEM],
        out_specs=VMEM,
        scratch_shapes=[pltpu.VMEM((256, 256), F32)],
        compiler_params=SMALL,
        name="other",
    )(core, other, right, own)
    mixed = exchange(back).reshape(1024, 128)
    out = pl.pallas_call(
        output_kernel,
        out_shape=shape((1024, 128), BF16),
        in_specs=[VMEM] * 3,
        out_specs=HBM,
        scratch_shapes=[
            pltpu.VMEM((1024, 128), F32),
            pltpu.VMEM((1024, 128), BF16),
            pltpu.SemaphoreType.DMA((8,)),
        ],
        compiler_params=SMALL,
        name="output",
    )(mixed, gate, out_weight)
    return out.reshape(pair.shape)


def solution(mesh):
    fine = Mesh(mesh.devices.reshape(2, 8, 2, 4, 2), ("xh", "z", "xl", "y", "core"))
    spec = P(("xh", "z"), ("xl", "y", "core"), None)
    in_specs = (spec, P(), P(), P(), P(), P(), P())
    return jax.shard_map(local, mesh=fine, in_specs=in_specs, out_specs=spec, check_vma=False)
```

```python
import functools
import itertools

import jax
import jax.numpy as jnp
from jax import lax
from jax.experimental import pallas as pl
from jax.experimental.pallas import tpu as pltpu
from jax.sharding import Mesh, PartitionSpec as P

EPSILON = 1e-05
AXES = ("xh", "z", "xl", "y", "core")
ROOT = (1, 5, 0, 2)


def hops(p, q):
    def ring(a, b, n):
        return min((a - b) % n, (b - a) % n)

    x = ring(2 * p[0] + p[2], 2 * q[0] + q[2], 4)
    return x + ring(p[1], q[1], 8) + ring(p[3], q[3], 4)


CHIPS = list(itertools.product(range(2), range(8), range(2), range(4)))
CHIPS.sort(key=lambda p: (p != ROOT, -hops(p, ROOT), p))
MEMBER = {p: n for n, p in enumerate(CHIPS)}
F32 = jnp.float32
BF16 = jnp.bfloat16
VMEM = pl.BlockSpec(memory_space=pltpu.VMEM)
SMEM = pl.BlockSpec(memory_space=pltpu.SMEM)
HBM = pl.BlockSpec(memory_space=pltpu.HBM)
SMALL = pltpu.CompilerParams(vmem_limit_bytes=12 << 20)


def swap_groups(v):
    lane = lax.broadcasted_iota(jnp.int32, v[0].shape, 1)
    low = lane < 64
    u = [None] * 4
    for c in (0, 1):
        a, b = v[c], v[c + 2]
        u[c] = jnp.where(low, a, pltpu.roll(b, 64, 1))
        u[c + 2] = jnp.where(low, pltpu.roll(a, 64, 1), b)
    even = (lane & 32) == 0
    out = [None] * 4
    for c in (0, 2):
        a, b = u[c], u[c + 1]
        out[c] = jnp.where(even, a, pltpu.roll(b, 32, 1))
        out[c + 1] = jnp.where(even, pltpu.roll(a, 96, 1), b)
    return out


def project_kernel(
    pair_hbm, gain_hbm, shift_hbm, w_hbm, gain_out_hbm, shift_out_hbm,
    msg_ref, normed_ref, aux_ref, w_gate_ref,
    pair_ref, w_ref, rows_ref, scr_ref, sem,
):
    def pair_copy(t):
        rows = pl.ds(t * 512, 512)
        return pltpu.make_async_copy(pair_hbm.at[rows], pair_ref.at[rows], sem.at[6 + t])

    small = [
        pltpu.make_async_copy(ref, rows_ref.at[pl.ds(t * 8, 1)], sem.at[t])
        for t, ref in enumerate((gain_hbm, shift_hbm, gain_out_hbm, shift_out_hbm))
    ]
    w_copy = pltpu.make_async_copy(w_hbm.at[:, pl.ds(0, 512)], w_ref, sem.at[4])
    w_gate_copy = pltpu.make_async_copy(w_hbm.at[:, pl.ds(512, 128)], w_gate_ref, sem.at[5])
    small[0].start()
    small[1].start()
    pair_copy(0).start()
    w_copy.start()
    pair_copy(1).start()
    small[2].start()
    small[3].start()
    w_gate_copy.start()
    small[0].wait()
    small[1].wait()
    gain = rows_ref[0:1, :]
    shift = rows_ref[8:9, :]

    def norm(t, carry):
        pair_copy(t).wait()
        for u in range(4):
            rows = pl.ds(pl.multiple_of(t * 512 + u * 128, 128), 128)
            x = pair_ref[rows, :].astype(F32)
            center = jnp.mean(x, axis=-1, keepdims=True)
            d = x - center
            spread = jnp.mean(d * d, axis=-1, keepdims=True)
            normed_ref[rows, :] = (d * lax.rsqrt(spread + EPSILON) * gain + shift).astype(BF16)
        return carry

    norm(0, 0)
    w_copy.wait()
    wt = jnp.transpose(w_ref[...])
    norm(1, 0)

    def step(t, carry):
        for u in range(2):
            n = normed_ref[pl.ds(pl.multiple_of(t * 512 + u * 256, 256), 256), :]
            p = lax.dot_general(wt, n, (((1,), (1,)), ((), ())), preferred_element_type=F32)
            left = jax.nn.sigmoid(p[0:128]) * p[128:256]
            right = jax.nn.sigmoid(p[256:384]) * p[384:512]
            for k in range(2):
                a = t * 4 + u * 2 + k
                lanes = slice(k * 128, (k + 1) * 128)
                scr_ref[pl.ds(a, 128, stride=16), :] = left[:, lanes]
                scr_ref[pl.ds(8 + a, 128, stride=16), :] = right[:, lanes]
        return carry

    for t in range(2):
        step(t, 0)

    def pack(t, carry):
        rows = pl.ds(pl.multiple_of(t * 512, 512), 512)
        msg_ref[rows, :] = scr_ref[rows, :].astype(BF16)
        return carry

    lax.fori_loop(0, 4, pack, 0)
    small[2].wait()
    small[3].wait()
    aux_ref[0:1, :] = rows_ref[16:17, :]
    aux_ref[8:9, :] = rows_ref[24:25, :]
    w_gate_copy.wait()


def spread_kernel(offset, recv_ref, out_ref):
    def step(xh, carry):
        for z in range(8):
            for xl in range(2):
                v = []
                for y in range(4):
                    low, high = (MEMBER[(t, z, xl, y)] for t in range(2))
                    start = pl.multiple_of((low + xh * (high - low)) * 16, 16)
                    piece = recv_ref[pl.ds(start, 16), :].astype(F32)
                    v.append(piece[offset : offset + 8])
                start = pl.multiple_of((xh * 8 + z) * 32, 32)
                out_ref[pl.ds(start, 32), xl * 128 : (xl + 1) * 128] = jnp.concatenate(
                    swap_groups(v), axis=0
                ).astype(BF16)
        return carry

    lax.fori_loop(0, 2, step, 0)


def multiply(left_ref, right_ref, mixed_ref):
    mixed_ref[...] = lax.dot_general(
        left_ref[...], right_ref[...], (((0,), (0,)), ((), ())), preferred_element_type=F32
    )


def member(xh, y, core, chip):
    a, b, c, d = (MEMBER[(t, 2 * y + u, *chip)] for t in range(2) for u in range(2))
    return a + xh * (c - a) + core * ((b - a) + xh * (a - b - c + d))


def pieces(mixed_ref, store, static=False):
    def step(xl, carry):
        for y in range(4):
            for g in range(2):
                v = []
                for b in range(4):
                    start = pl.multiple_of((xl * 4 + y) * 32 + b * 8, 8)
                    v.append(mixed_ref[pl.ds(start, 8), g * 128 : (g + 1) * 128])
                store(xl, y, g, swap_groups(v))
        return carry

    if static:
        for t in range(2):
            step(t, 0)
    else:
        lax.fori_loop(0, 2, step, 0)


def own_kernel(
    recv_ref, left_ref, normed_ref, aux_ref, w_gate_ref, right_ref, out_ref, gate_ref, mixed_ref
):
    spread_kernel(8, recv_ref, right_ref)
    multiply(left_ref, right_ref, mixed_ref)
    gate_ref[0:1024, :] = jax.nn.sigmoid(
        jnp.dot(normed_ref[...], w_gate_ref[...], preferred_element_type=F32)
    )

    def store(xl, y, g, v):
        start = pl.multiple_of(((xl * 4 + y) * 2 + g) * 32, 32)
        out_ref[pl.ds(start, 32), :] = jnp.concatenate(v, axis=0).astype(BF16)

    pieces(mixed_ref, store)
    for k in range(2):
        gate_ref[1024 + 128 * k : 1152 + 128 * k, :] = jnp.transpose(
            jnp.broadcast_to(aux_ref[8 * k : 8 * k + 1, :], (128, 128))
        )


def other_kernel(core_ref, left_ref, right_ref, own_ref, out_ref, mixed_ref):
    core = core_ref[0]
    multiply(left_ref, right_ref, mixed_ref)

    def store(xl, y, g, v):
        for c in range(4):
            start = pl.multiple_of((xl * 4 + y) * 64 + (g * 4 + c) * 8, 8)
            out_ref[member(xl, y, core, (g, c))] = own_ref[pl.ds(start, 8), :]
            out_ref[member(xl, y, 1 - core, (g, c))] = v[c].astype(BF16)

    pieces(mixed_ref, store, True)


def output_kernel(recv_ref, gate_ref, w_ref, out_hbm, scr_ref, out_ref, sem):
    def out_copy(half, b):
        rows = pl.ds((b * 8 + half * 4) * 32, 128)
        return pltpu.make_async_copy(out_ref.at[rows], out_hbm.at[rows], sem.at[half * 4 + b])

    def total_step(t, sums):
        sums = list(sums)
        for u in range(16):
            rows = pl.ds(t * 256 + u * 16, 16)
            x = recv_ref[rows, :].astype(F32)
            scr_ref[rows, :] = x
            sums[u % 4] = sums[u % 4] + (x[0:8] + x[8:16])
        return tuple(sums)

    zero = jnp.zeros((8, 128), F32)
    sums = (zero,) * 4
    for t in range(4):
        sums = total_step(t, sums)
    center = ((sums[0] + sums[1]) + (sums[2] + sums[3])) * (1.0 / 128.0)

    def square_step(t, sums):
        sums = list(sums)
        for u in range(32):
            d = scr_ref[pl.ds(t * 256 + u * 8, 8), :] - center
            sums[u % 4] = sums[u % 4] + d * d
        return tuple(sums)

    sums = (zero,) * 4
    for t in range(4):
        sums = square_step(t, sums)
    spread = ((sums[0] + sums[1]) + (sums[2] + sums[3])) * (1.0 / 128.0)
    scale = lax.rsqrt(spread + EPSILON)
    w = w_ref[...]
    gain = gate_ref[1024:1152, :]
    shift = gate_ref[1152:1280, :]
    for s in range(8):
        x = scr_ref[pl.ds(s, 128, stride=8), :]
        x = (x - center[s : s + 1]) * scale[s : s + 1] * gain + shift
        o = lax.dot_general(
            x.astype(BF16), w, (((0,), (0,)), ((), ())), preferred_element_type=F32
        )
        for b in range(4):
            i = b * 8 + s
            rows = slice(i * 32, (i + 1) * 32)
            out_ref[rows, :] = (gate_ref[rows, :] * o[b * 32 : (b + 1) * 32]).astype(BF16)
        if s % 4 == 3:
            for b in range(4):
                out_copy(s // 4, b).start()
    for half in range(2):
        for b in range(4):
            out_copy(half, b).wait()


def chip_groups():
    return [
        [(((xh * 8 + z) * 2 + xl) * 4 + y) * 2 + core for xh, z, xl, y in CHIPS]
        for core in range(2)
    ]


def exchange(x):
    return lax.all_to_all(x, AXES, 0, 0, axis_index_groups=chip_groups(), tiled=True)


def local(pair, norm_in, shift_in, in_weight, norm_out, shift_out, out_weight):
    core = lax.axis_index("core").astype(jnp.int32).reshape(1)
    shape = jax.ShapeDtypeStruct
    stay = functools.partial(pltpu.with_memory_space_constraint, memory_space=pltpu.HBM)
    msg, normed, aux, w_gate = pl.pallas_call(
        project_kernel,
        out_shape=(
            shape((2048, 128), BF16),
            shape((1024, 128), BF16),
            shape((16, 128), F32),
            shape((128, 128), BF16),
        ),
        in_specs=[HBM] * 6,
        out_specs=(VMEM,) * 4,
        scratch_shapes=[
            pltpu.VMEM((1024, 128), BF16),
            pltpu.VMEM((128, 512), BF16),
            pltpu.VMEM((32, 128), F32),
            pltpu.VMEM((2048, 128), F32),
            pltpu.SemaphoreType.DMA((8,)),
        ],
        compiler_params=SMALL,
        name="project",
    )(
        stay(pair.reshape(1024, 128)),
        stay(norm_in.reshape(1, 128)),
        stay(shift_in.reshape(1, 128)),
        stay(in_weight),
        stay(norm_out.reshape(1, 128)),
        stay(shift_out.reshape(1, 128)),
    )
    recv = exchange(msg.reshape(128, 16, 128)).reshape(2048, 128)
    left = pl.pallas_call(
        functools.partial(spread_kernel, 0),
        out_shape=shape((512, 256), BF16),
        in_specs=[VMEM],
        out_specs=VMEM,
        compiler_params=SMALL,
        name="spread",
    )(recv)
    other = lax.ppermute(left, "core", [(0, 1), (1, 0)])
    right, own, gate = pl.pallas_call(
        own_kernel,
        out_shape=(shape((512, 256), BF16), shape((512, 128), BF16), shape((1280, 128), F32)),
        in_specs=[VMEM] * 5,
        out_specs=(VMEM,) * 3,
        scratch_shapes=[pltpu.VMEM((256, 256), F32)],
        compiler_params=SMALL,
        name="own",
        cost_estimate=pl.CostEstimate(flops=1 << 26, bytes_accessed=1 << 20, transcendentals=0),
    )(recv, left, normed, aux, w_gate)
    back = pl.pallas_call(
        other_kernel,
        out_shape=shape((128, 8, 128), BF16),
        in_specs=[SMEM, VMEM, VMEM, VMEM],
        out_specs=VMEM,
        scratch_shapes=[pltpu.VMEM((256, 256), F32)],
        compiler_params=SMALL,
        name="other",
    )(core, other, right, own)
    mixed = exchange(back).reshape(1024, 128)
    out = pl.pallas_call(
        output_kernel,
        out_shape=shape((1024, 128), BF16),
        in_specs=[VMEM] * 3,
        out_specs=HBM,
        scratch_shapes=[
            pltpu.VMEM((1024, 128), F32),
            pltpu.VMEM((1024, 128), BF16),
            pltpu.SemaphoreType.DMA((8,)),
        ],
        compiler_params=SMALL,
        name="output",
    )(mixed, gate, out_weight)
    return out.reshape(pair.shape)


def solution(mesh):
    fine = Mesh(mesh.devices.reshape(2, 8, 2, 4, 2), ("xh", "z", "xl", "y", "core"))
    spec = P(("xh", "z"), ("xl", "y", "core"), None)
    in_specs = (spec, P(), P(), P(), P(), P(), P())
    return jax.shard_map(local, mesh=fine, in_specs=in_specs, out_specs=spec, check_vma=False)
```

```python
import functools
import itertools

import jax
import jax.numpy as jnp
from jax import lax
from jax.experimental import pallas as pl
from jax.experimental.pallas import tpu as pltpu
from jax.sharding import Mesh, PartitionSpec as P

EPSILON = 1e-05
AXES = ("xh", "z", "xl", "y", "core")
ROOT = (1, 5, 0, 2)


def hops(p, q):
    def ring(a, b, n):
        return min((a - b) % n, (b - a) % n)

    x = ring(2 * p[0] + p[2], 2 * q[0] + q[2], 4)
    return x + ring(p[1], q[1], 8) + ring(p[3], q[3], 4)


CHIPS = list(itertools.product(range(2), range(8), range(2), range(4)))
CHIPS.sort(key=lambda p: (p != ROOT, -hops(p, ROOT), p))
MEMBER = {p: n for n, p in enumerate(CHIPS)}
F32 = jnp.float32
BF16 = jnp.bfloat16
VMEM = pl.BlockSpec(memory_space=pltpu.VMEM)
SMEM = pl.BlockSpec(memory_space=pltpu.SMEM)
HBM = pl.BlockSpec(memory_space=pltpu.HBM)
SMALL = pltpu.CompilerParams(vmem_limit_bytes=12 << 20)


def swap_groups(v):
    lane = lax.broadcasted_iota(jnp.int32, v[0].shape, 1)
    low = lane < 64
    u = [None] * 4
    for c in (0, 1):
        a, b = v[c], v[c + 2]
        u[c] = jnp.where(low, a, pltpu.roll(b, 64, 1))
        u[c + 2] = jnp.where(low, pltpu.roll(a, 64, 1), b)
    even = (lane & 32) == 0
    out = [None] * 4
    for c in (0, 2):
        a, b = u[c], u[c + 1]
        out[c] = jnp.where(even, a, pltpu.roll(b, 32, 1))
        out[c + 1] = jnp.where(even, pltpu.roll(a, 96, 1), b)
    return out


def project_kernel(
    pair_hbm, gain_hbm, shift_hbm, w_hbm, gain_out_hbm, shift_out_hbm,
    msg_ref, normed_ref, aux_ref, w_gate_ref,
    pair_ref, w_ref, rows_ref, scr_ref, sem,
):
    def pair_copy(t):
        rows = pl.ds(t * 512, 512)
        return pltpu.make_async_copy(pair_hbm.at[rows], pair_ref.at[rows], sem.at[6 + t])

    small = [
        pltpu.make_async_copy(ref, rows_ref.at[pl.ds(t * 8, 1)], sem.at[t])
        for t, ref in enumerate((gain_hbm, shift_hbm, gain_out_hbm, shift_out_hbm))
    ]
    w_copy = pltpu.make_async_copy(w_hbm.at[:, pl.ds(0, 512)], w_ref, sem.at[4])
    w_gate_copy = pltpu.make_async_copy(w_hbm.at[:, pl.ds(512, 128)], w_gate_ref, sem.at[5])
    pair_copy(0).start()
    small[0].start()
    small[1].start()
    w_copy.start()
    pair_copy(1).start()
    small[2].start()
    small[3].start()
    w_gate_copy.start()
    small[0].wait()
    small[1].wait()
    gain = rows_ref[0:1, :]
    shift = rows_ref[8:9, :]

    def norm(t, carry):
        pair_copy(t).wait()
        for u in range(4):
            rows = pl.ds(pl.multiple_of(t * 512 + u * 128, 128), 128)
            x = pair_ref[rows, :].astype(F32)
            center = jnp.mean(x, axis=-1, keepdims=True)
            d = x - center
            spread = jnp.mean(d * d, axis=-1, keepdims=True)
            normed_ref[rows, :] = (d * lax.rsqrt(spread + EPSILON) * gain + shift).astype(BF16)
        return carry

    norm(0, 0)
    w_copy.wait()
    wt = jnp.transpose(w_ref[...])
    norm(1, 0)

    def step(t, carry):
        for u in range(1):
            n = normed_ref[pl.ds(t * 512, 512), :]
            p = lax.dot_general(wt, n, (((1,), (1,)), ((), ())), preferred_element_type=F32)
            left = jax.nn.sigmoid(p[0:128]) * p[128:256]
            right = jax.nn.sigmoid(p[256:384]) * p[384:512]
            for k in range(4):
                a = t * 4 + k
                lanes = slice(k * 128, (k + 1) * 128)
                scr_ref[pl.ds(a, 128, stride=16), :] = left[:, lanes]
                scr_ref[pl.ds(8 + a, 128, stride=16), :] = right[:, lanes]
        return carry

    for t in range(2):
        step(t, 0)

    def pack(t, carry):
        rows = pl.ds(pl.multiple_of(t * 512, 512), 512)
        msg_ref[rows, :] = scr_ref[rows, :].astype(BF16)
        return carry

    lax.fori_loop(0, 4, pack, 0)
    small[2].wait()
    small[3].wait()
    aux_ref[0:1, :] = rows_ref[16:17, :]
    aux_ref[8:9, :] = rows_ref[24:25, :]
    w_gate_copy.wait()


def spread_kernel(offset, recv_ref, out_ref):
    def step(xh, carry):
        for z in range(8):
            for xl in range(2):
                v = []
                for y in range(4):
                    low, high = (MEMBER[(t, z, xl, y)] for t in range(2))
                    start = pl.multiple_of((low + xh * (high - low)) * 16, 16)
                    piece = recv_ref[pl.ds(start, 16), :].astype(F32)
                    v.append(piece[offset : offset + 8])
                start = pl.multiple_of((xh * 8 + z) * 32, 32)
                out_ref[pl.ds(start, 32), xl * 128 : (xl + 1) * 128] = jnp.concatenate(
                    swap_groups(v), axis=0
                ).astype(BF16)
        return carry

    lax.fori_loop(0, 2, step, 0)


def multiply(left_ref, right_ref, mixed_ref):
    mixed_ref[...] = lax.dot_general(
        left_ref[...], right_ref[...], (((0,), (0,)), ((), ())), preferred_element_type=F32
    )


def member(xh, y, core, chip):
    a, b, c, d = (MEMBER[(t, 2 * y + u, *chip)] for t in range(2) for u in range(2))
    return a + xh * (c - a) + core * ((b - a) + xh * (a - b - c + d))


def pieces(mixed_ref, store, static=False):
    def step(xl, carry):
        for y in range(4):
            for g in range(2):
                v = []
                for b in range(4):
                    start = pl.multiple_of((xl * 4 + y) * 32 + b * 8, 8)
                    v.append(mixed_ref[pl.ds(start, 8), g * 128 : (g + 1) * 128])
                store(xl, y, g, swap_groups(v))
        return carry

    if static:
        for t in range(2):
            step(t, 0)
    else:
        lax.fori_loop(0, 2, step, 0)


def own_kernel(
    recv_ref, left_ref, normed_ref, aux_ref, w_gate_ref, right_ref, out_ref, gate_ref, mixed_ref
):
    spread_kernel(8, recv_ref, right_ref)
    multiply(left_ref, right_ref, mixed_ref)
    gate_ref[0:1024, :] = jax.nn.sigmoid(
        jnp.dot(normed_ref[...], w_gate_ref[...], preferred_element_type=F32)
    )

    def store(xl, y, g, v):
        start = pl.multiple_of(((xl * 4 + y) * 2 + g) * 32, 32)
        out_ref[pl.ds(start, 32), :] = jnp.concatenate(v, axis=0).astype(BF16)

    pieces(mixed_ref, store)
    for k in range(2):
        gate_ref[1024 + 128 * k : 1152 + 128 * k, :] = jnp.transpose(
            jnp.broadcast_to(aux_ref[8 * k : 8 * k + 1, :], (128, 128))
        )


def other_kernel(core_ref, left_ref, right_ref, own_ref, out_ref, mixed_ref):
    core = core_ref[0]
    multiply(left_ref, right_ref, mixed_ref)

    def store(xl, y, g, v):
        for c in range(4):
            start = pl.multiple_of((xl * 4 + y) * 64 + (g * 4 + c) * 8, 8)
            out_ref[member(xl, y, core, (g, c))] = own_ref[pl.ds(start, 8), :]
            out_ref[member(xl, y, 1 - core, (g, c))] = v[c].astype(BF16)

    pieces(mixed_ref, store, True)


def output_kernel(recv_ref, gate_ref, w_ref, out_hbm, scr_ref, out_ref, sem):
    def out_copy(half, b):
        rows = pl.ds((b * 8 + half * 4) * 32, 128)
        return pltpu.make_async_copy(out_ref.at[rows], out_hbm.at[rows], sem.at[half * 4 + b])

    def total_step(t, sums):
        sums = list(sums)
        for u in range(16):
            rows = pl.ds(t * 256 + u * 16, 16)
            x = recv_ref[rows, :].astype(F32)
            scr_ref[rows, :] = x
            sums[u % 4] = sums[u % 4] + (x[0:8] + x[8:16])
        return tuple(sums)

    zero = jnp.zeros((8, 128), F32)
    sums = (zero,) * 4
    for t in range(4):
        sums = total_step(t, sums)
    center = ((sums[0] + sums[1]) + (sums[2] + sums[3])) * (1.0 / 128.0)

    def square_step(t, sums):
        sums = list(sums)
        for u in range(32):
            d = scr_ref[pl.ds(t * 256 + u * 8, 8), :] - center
            sums[u % 4] = sums[u % 4] + d * d
        return tuple(sums)

    sums = (zero,) * 4
    for t in range(4):
        sums = square_step(t, sums)
    spread = ((sums[0] + sums[1]) + (sums[2] + sums[3])) * (1.0 / 128.0)
    scale = lax.rsqrt(spread + EPSILON)
    w = w_ref[...]
    gain = gate_ref[1024:1152, :]
    shift = gate_ref[1152:1280, :]
    for s in range(8):
        x = scr_ref[pl.ds(s, 128, stride=8), :]
        x = (x - center[s : s + 1]) * scale[s : s + 1] * gain + shift
        o = lax.dot_general(
            x.astype(BF16), w, (((0,), (0,)), ((), ())), preferred_element_type=F32
        )
        for b in range(4):
            i = b * 8 + s
            rows = slice(i * 32, (i + 1) * 32)
            out_ref[rows, :] = (gate_ref[rows, :] * o[b * 32 : (b + 1) * 32]).astype(BF16)
        if s % 4 == 3:
            for b in range(4):
                out_copy(s // 4, b).start()
    for half in range(2):
        for b in range(4):
            out_copy(half, b).wait()


def chip_groups():
    return [
        [(((xh * 8 + z) * 2 + xl) * 4 + y) * 2 + core for xh, z, xl, y in CHIPS]
        for core in range(2)
    ]


def exchange(x):
    return lax.all_to_all(x, AXES, 0, 0, axis_index_groups=chip_groups(), tiled=True)


def local(pair, norm_in, shift_in, in_weight, norm_out, shift_out, out_weight):
    core = lax.axis_index("core").astype(jnp.int32).reshape(1)
    shape = jax.ShapeDtypeStruct
    stay = functools.partial(pltpu.with_memory_space_constraint, memory_space=pltpu.HBM)
    msg, normed, aux, w_gate = pl.pallas_call(
        project_kernel,
        out_shape=(
            shape((2048, 128), BF16),
            shape((1024, 128), BF16),
            shape((16, 128), F32),
            shape((128, 128), BF16),
        ),
        in_specs=[HBM] * 6,
        out_specs=(VMEM,) * 4,
        scratch_shapes=[
            pltpu.VMEM((1024, 128), BF16),
            pltpu.VMEM((128, 512), BF16),
            pltpu.VMEM((32, 128), F32),
            pltpu.VMEM((2048, 128), F32),
            pltpu.SemaphoreType.DMA((8,)),
        ],
        compiler_params=SMALL,
        name="project",
    )(
        stay(pair.reshape(1024, 128)),
        stay(norm_in.reshape(1, 128)),
        stay(shift_in.reshape(1, 128)),
        stay(in_weight),
        stay(norm_out.reshape(1, 128)),
        stay(shift_out.reshape(1, 128)),
    )
    recv = exchange(msg.reshape(128, 16, 128)).reshape(2048, 128)
    left = pl.pallas_call(
        functools.partial(spread_kernel, 0),
        out_shape=shape((512, 256), BF16),
        in_specs=[VMEM],
        out_specs=VMEM,
        compiler_params=SMALL,
        name="spread",
    )(recv)
    other = lax.ppermute(left, "core", [(0, 1), (1, 0)])
    right, own, gate = pl.pallas_call(
        own_kernel,
        out_shape=(shape((512, 256), BF16), shape((512, 128), BF16), shape((1280, 128), F32)),
        in_specs=[VMEM] * 5,
        out_specs=(VMEM,) * 3,
        scratch_shapes=[pltpu.VMEM((256, 256), F32)],
        compiler_params=SMALL,
        name="own",
        cost_estimate=pl.CostEstimate(flops=1 << 26, bytes_accessed=1 << 20, transcendentals=0),
    )(recv, left, normed, aux, w_gate)
    back = pl.pallas_call(
        other_kernel,
        out_shape=shape((128, 8, 128), BF16),
        in_specs=[SMEM, VMEM, VMEM, VMEM],
        out_specs=VMEM,
        scratch_shapes=[pltpu.VMEM((256, 256), F32)],
        compiler_params=SMALL,
        name="other",
    )(core, other, right, own)
    mixed = exchange(back).reshape(1024, 128)
    out = pl.pallas_call(
        output_kernel,
        out_shape=shape((1024, 128), BF16),
        in_specs=[VMEM] * 3,
        out_specs=HBM,
        scratch_shapes=[
            pltpu.VMEM((1024, 128), F32),
            pltpu.VMEM((1024, 128), BF16),
            pltpu.SemaphoreType.DMA((8,)),
        ],
        compiler_params=SMALL,
        name="output",
    )(mixed, gate, out_weight)
    return out.reshape(pair.shape)


def solution(mesh):
    fine = Mesh(mesh.devices.reshape(2, 8, 2, 4, 2), ("xh", "z", "xl", "y", "core"))
    spec = P(("xh", "z"), ("xl", "y", "core"), None)
    in_specs = (spec, P(), P(), P(), P(), P(), P())
    return jax.shard_map(local, mesh=fine, in_specs=in_specs, out_specs=spec, check_vma=False)
```
